32 devices in a mesh: grp: 4 (over z), seq: 8 (over y, x, core).
Axes of the slice: x: 2, y: 2, z: 4, core: 2. Of those that a mesh axis runs over, the one named last changes fastest.
Arguments:
- hidden_in: bfloat16 [24, 4096], P(None, ('grp', 'seq')), may hold values from -6 to 6
- norm_gain: float32 [4096], replicated, may hold values from 0.5 to 1.5
- w_ssm_in: bfloat16 [4096, 8192], P(None, ('grp', 'seq')), may hold values from -0.09375 to 0.09375
- w_ssm_gate: bfloat16 [4096, 8192], P(None, ('grp', 'seq')), may hold values from -0.09375 to 0.09375
- conv_weight: float32 [4, 8192], P(None, ('grp', 'seq')), may hold values from -3 to 3
- conv_bias: float32 [8192], P(('grp', 'seq')), may hold values from -0.5 to 0.5
- conv_state: bfloat16 [24, 3, 8192], P(None, None, ('grp', 'seq')), may hold values from -6 to 6
- w_state_proj: bfloat16 [8192, 288], P(('grp', 'seq')), may hold values from -0.0625 to 0.0625
- w_step: bfloat16 [256, 8192], P(None, ('grp', 'seq')), may hold values from -0.375 to 0.375
- step_bias: float32 [8192], P(('grp', 'seq')), may hold values from -4 to -1
- log_decay: float32 [16, 8192], P(None, ('grp', 'seq')), may hold values from 0 to 2.7
- skip_gain: float32 [8192], P(('grp', 'seq')), may hold values from 0.5 to 1.5
- ssm_state: float32 [24, 16, 8192], P(None, None, ('grp', 'seq')), may hold values from -6 to 6
- w_ssm_out: bfloat16 [8192, 4096], P(('grp', 'seq')), may hold values from -0.125 to 0.125
- w_query: bfloat16 [4096, 2048], P(None, 'grp'), may hold values from -6 to 6
- key_projection: bfloat16 [4096, 1024], P(None, 'grp'), may hold values from -0.09375 to 0.09375
- value_projection: bfloat16 [4096, 1024], P(None, 'grp'), may hold values from -0.09375 to 0.09375
- w_attn_out: bfloat16 [2048, 4096], P('grp', 'seq'), may hold values from -0.125 to 0.125
- w_mlp_gate: bfloat16 [4096, 14336], P(None, ('grp', 'seq')), may hold values from -0.09375 to 0.09375
- w_mlp_up: bfloat16 [4096, 14336], P(None, ('grp', 'seq')), may hold values from -0.09375 to 0.09375
- w_mlp_down: bfloat16 [14336, 4096], P(('grp', 'seq')), may hold values from -0.09375 to 0.09375
- cached_inputs: bfloat16 [24, 512, 4096], P('seq'), may hold values from -6 to 6
- window_lengths: int32 [24], replicated, may hold values from 1 to 512, as said below
Outputs:
- hidden_out: bfloat16 [24, 4096], P(None, ('grp', 'seq'))
- state_out: float32 [24, 16, 8192], P(None, None, ('grp', 'seq'))
The draws below stay inside these ranges and needn't reach their ends.
Inputs may be any that keep to these rules, and one draw needn't show every extreme that they name: `window_lengths`: every sequence has at least one valid cached position, and some sequence fills the whole window of 512.
All inputs are finite; a program needn't handle non-finite values.
Results may differ from the reference program's by a relative error of at most 0.012.
The reference program's roundings to bfloat16 on the way count: a program that leaves them out, or rounds other values in their place, can miss the bound.
Values may be sent and summed in bfloat16 or wider, within the bound.
No kernel may reach another device: no remote copies, remote signals or barrier semaphores. Data moves between devices by JAX's collectives and lax.ppermute only.
A program may use at most 128 MiB of HBM per device.

```python
import jax
import jax.numpy as jnp
from jax import lax

MODEL_DIM = 4096
E = 8192
NS = 16
KC = 4
DTR = 256
QUERY_HEADS = 16
KEY_VALUE_HEADS = 8
HEAD_SIZE = 128
FF = 14336
WINDOW_SPAN = 512
BATCH_SEQUENCES = 24


def draw_window_lengths(key, part):
    drawn_lengths = jax.random.randint(jax.random.fold_in(key, 7), (BATCH_SEQUENCES,), 1, WINDOW_SPAN + 1, dtype=jnp.int32)
    chosen = jax.random.randint(jax.random.fold_in(key, 11), (), 0, BATCH_SEQUENCES, dtype=jnp.int32)
    return jnp.where(jnp.arange(BATCH_SEQUENCES, dtype=jnp.int32) == chosen, WINDOW_SPAN, drawn_lengths).astype(jnp.int32)


def draw_w_query(key, part):
    columns = QUERY_HEADS * HEAD_SIZE
    chosen_heads = jax.random.permutation(jax.random.fold_in(key, 3), QUERY_HEADS)
    entries = jax.random.normal(jax.random.fold_in(key, 5), (MODEL_DIM, columns), jnp.float32)
    levels = jnp.array([24.0, 48.0, 96.0], jnp.float32)
    head_scale = jnp.ones((QUERY_HEADS,), jnp.float32).at[chosen_heads[:3]].set(levels)
    column_scale = jnp.repeat(head_scale, HEAD_SIZE)
    scaled = entries * column_scale[None, :] * float(MODEL_DIM) ** (-0.5)
    return jnp.clip(scaled, -6.0, 6.0).astype(jnp.bfloat16)


def spiked(values, key, source, target, blocks, factor):
    def block_of(axis_at):
        return (jnp.arange(values.shape[axis_at]) // (values.shape[axis_at] // blocks)).reshape((-1,) + (1,) * (values.ndim - 1 - axis_at))

    one_side = jax.random.permutation(key, blocks)[block_of(target)]
    far = (block_of(target) + blocks // 2) % blocks
    return jnp.where((block_of(source) == one_side) | (block_of(source) == far), factor * values, values)


def level_of(stream_key, dims, shards, least, high):
    loudness, own = 1.0, jax.random.fold_in(stream_key, 6)
    for dim, shards_of in shards:
        draws = jnp.exp(jax.random.uniform(jax.random.fold_in(own, dim), (shards_of,), jnp.float32, least / len(shards), high / len(shards)))
        loudness = loudness * jnp.repeat(draws, dims[dim] // shards_of).reshape([-1 if axis == dim else 1 for axis in range(len(dims))])
    return loudness


def bell_draw(stream_key, dims, scale, reach, pieces=(), held_as=jnp.bfloat16):
    level = level_of(stream_key, dims, pieces, -0.22, 0.18) if pieces else 1.0
    values = jax.random.normal(stream_key, dims, jnp.float32) * scale * level
    return jnp.minimum(jnp.maximum(values, -reach), reach).astype(held_as)


def noise_with(rng, extent, deviation, limit, shards, heavy, kind=jnp.bfloat16):
    drawn = deviation * jax.random.normal(rng, extent, jnp.float32)
    if shards:
        drawn = drawn * level_of(rng, extent, shards, -0.22, 0.18)
    return jnp.clip(spiked(drawn, jax.random.fold_in(rng, 3), *heavy), -limit, limit).astype(kind)


def setup_inputs(seed: int = 0) -> dict:
    key_list = jax.random.split(jax.random.key(seed), 24)
    return {
        "hidden_in": bell_draw(key_list[0], (BATCH_SEQUENCES, MODEL_DIM), 1.0, 6.0, ((1, 32),)),
        "norm_gain": jnp.clip(1.0 + 0.1 * jax.random.normal(key_list[1], (MODEL_DIM,), jnp.float32), 0.5, 1.5),
        "w_ssm_in": bell_draw(key_list[2], (MODEL_DIM, E), MODEL_DIM ** -0.5, 0.09375, ((1, 32),)),
        "w_ssm_gate": bell_draw(key_list[3], (MODEL_DIM, E), MODEL_DIM ** -0.5, 0.09375, ((1, 32),)),
        "conv_weight": bell_draw(key_list[4], (KC, E), KC ** -0.5, 3.0, ((1, 32),), jnp.float32),
        "conv_bias": jnp.clip(jax.random.uniform(key_list[5], (E,), jnp.float32, -0.5, 0.5) * level_of(key_list[5], (E,), ((0, 32),), -0.4, 0.0), -0.5, 0.5),
        "conv_state": bell_draw(key_list[6], (BATCH_SEQUENCES, KC - 1, E), 1.0, 6.0, ((2, 32),)),
        "w_state_proj": bell_draw(key_list[7], (E, DTR + 2 * NS), E ** -0.5, 0.0625, ((0, 32),)),
        "w_step": bell_draw(key_list[8], (DTR, E), DTR ** -0.5, 0.375, ((1, 32),)),
        "step_bias": jnp.clip(-4.0 + 3.0 * jax.random.uniform(key_list[9], (E,), jnp.float32) ** level_of(key_list[9], (E,), ((0, 32),), -0.2, 0.2), -4.0, -1.0),
        "log_decay": jnp.clip(2.7 * jax.random.uniform(key_list[10], (NS, E), jnp.float32) ** level_of(key_list[10], (NS, E), ((1, 32),), -0.2, 0.2), 0.0, 2.7),
        "skip_gain": jnp.clip(0.5 + 1.0 * jax.random.uniform(key_list[11], (E,), jnp.float32) ** level_of(key_list[11], (E,), ((0, 32),), -0.2, 0.2), 0.5, 1.5),
        "ssm_state": bell_draw(key_list[12], (BATCH_SEQUENCES, NS, E), 1.0, 6.0, ((2, 32),), jnp.float32),
        "w_ssm_out": noise_with(key_list[13], (E, MODEL_DIM), E ** -0.5, 0.125, ((0, 32),), (0, 1, 32, 2.75)),
        "w_query": draw_w_query(jax.random.fold_in(key_list[23], 71), 0),
        "key_projection": bell_draw(key_list[15], (MODEL_DIM, KEY_VALUE_HEADS * HEAD_SIZE), MODEL_DIM ** -0.5, 0.09375, ((1, 4),)),
        "value_projection": bell_draw(key_list[16], (MODEL_DIM, KEY_VALUE_HEADS * HEAD_SIZE), MODEL_DIM ** -0.5, 0.09375, ((1, 4),)),
        "w_attn_out": bell_draw(key_list[17], (QUERY_HEADS * HEAD_SIZE, MODEL_DIM), (QUERY_HEADS * HEAD_SIZE) ** -0.5, 0.125, ((0, 4), (1, 8))),
        "w_mlp_gate": bell_draw(key_list[18], (MODEL_DIM, FF), MODEL_DIM ** -0.5, 0.09375, ((1, 32),)),
        "w_mlp_up": bell_draw(key_list[19], (MODEL_DIM, FF), MODEL_DIM ** -0.5, 0.09375, ((1, 32),)),
        "w_mlp_down": noise_with(key_list[20], (FF, MODEL_DIM), FF ** -0.5, 0.09375, ((0, 32),), (0, 1, 32, 2.75)),
        "cached_inputs": bell_draw(key_list[21], (BATCH_SEQUENCES, WINDOW_SPAN, MODEL_DIM), 1.0, 6.0, ((0, 8),)),
        "window_lengths": draw_window_lengths(jax.random.fold_in(key_list[23], 71), 0),
    }


epsilon = 1e-05
rope_base = 10000.0

def apply_rotary(head_values, positions):
    half_dim = head_values.shape[-1] // 2
    frequency = rope_base ** (-(jnp.arange(half_dim, dtype=jnp.float32) * 2.0) / head_values.shape[-1])
    angles = positions[..., None, None] * frequency
    cosine = jnp.cos(angles)
    sine_part = jnp.sin(angles)
    front_half = head_values[..., :half_dim]
    back_half = head_values[..., half_dim:]
    return jnp.concatenate([front_half * cosine - back_half * sine_part, back_half * cosine + front_half * sine_part], axis=-1)

def reference(hidden_in, norm_gain, w_ssm_in, w_ssm_gate, conv_weight, conv_bias, conv_state, w_state_proj, w_step, step_bias, log_decay, skip_gain, ssm_state, w_ssm_out, w_query, key_projection, value_projection, w_attn_out, w_mlp_gate, w_mlp_up, w_mlp_down, cached_inputs, window_lengths):
    hidden_f = hidden_in.astype(jnp.float32)
    row_scale = lax.rsqrt(lax.optimization_barrier(jnp.mean(hidden_f * hidden_f, axis=1, keepdims=True)) + epsilon)
    normed_input = (hidden_f * row_scale * norm_gain).astype(jnp.bfloat16)
    ssm_input = jnp.dot(normed_input, w_ssm_in, preferred_element_type=jnp.float32).astype(jnp.bfloat16)
    gate_input = jnp.dot(normed_input, w_ssm_gate, preferred_element_type=jnp.float32)
    past_inputs = conv_state.astype(jnp.float32)
    conv_sum = conv_bias + lax.optimization_barrier(jnp.sum(past_inputs * conv_weight[:-1][None], axis=1)) + conv_weight[-1] * lax.optimization_barrier(ssm_input).astype(jnp.float32)
    conv_out = jax.nn.silu(conv_sum)
    low_rank = jnp.dot(conv_out.astype(jnp.bfloat16), w_state_proj, preferred_element_type=jnp.float32)
    step_low = low_rank[:, :DTR].astype(jnp.bfloat16)
    input_map = low_rank[:, DTR:DTR + NS]
    output_map = low_rank[:, DTR + NS:]
    step_size = jax.nn.softplus(jnp.dot(step_low, w_step, preferred_element_type=jnp.float32) + step_bias)
    decay_rate = jnp.exp(log_decay)
    state_out = jnp.exp(-step_size[:, None, :] * decay_rate[None]) * ssm_state + step_size[:, None, :] * input_map[:, :, None] * conv_out[:, None, :]
    ssm_mixed = lax.optimization_barrier(jnp.sum(state_out * output_map[:, :, None], axis=1)) + skip_gain * conv_out
    ssm_gated = (ssm_mixed * jax.nn.silu(gate_input)).astype(jnp.bfloat16)
    ssm_term = jnp.dot(ssm_gated, w_ssm_out, preferred_element_type=jnp.float32)
    gate_act = jnp.dot(normed_input, w_mlp_gate, preferred_element_type=jnp.float32)
    up_act = jnp.dot(normed_input, w_mlp_up, preferred_element_type=jnp.float32)
    mlp_hidden = (jax.nn.silu(gate_act) * up_act).astype(jnp.bfloat16)
    mlp_term = jnp.dot(mlp_hidden, w_mlp_down, preferred_element_type=jnp.float32)
    fresh_position = window_lengths.astype(jnp.float32)
    query = apply_rotary(jnp.dot(normed_input, w_query, preferred_element_type=jnp.float32).reshape(BATCH_SEQUENCES, QUERY_HEADS, HEAD_SIZE), fresh_position).astype(jnp.bfloat16)
    fresh_key = apply_rotary(jnp.dot(normed_input, key_projection, preferred_element_type=jnp.float32).reshape(BATCH_SEQUENCES, KEY_VALUE_HEADS, HEAD_SIZE), fresh_position).astype(jnp.bfloat16)
    fresh_value = jnp.dot(normed_input, value_projection, preferred_element_type=jnp.float32).astype(jnp.bfloat16).reshape(BATCH_SEQUENCES, KEY_VALUE_HEADS, HEAD_SIZE)
    heads_per_group = QUERY_HEADS // KEY_VALUE_HEADS
    attention_scale = HEAD_SIZE ** (-0.5)

    def one_row(row_args):
        window_row_inputs, query_for_row, row_key, row_value, row_length = row_args
        slot_ids = jnp.arange(WINDOW_SPAN, dtype=jnp.int32)
        window_key_rows = jnp.dot(window_row_inputs, key_projection, preferred_element_type=jnp.float32).reshape(WINDOW_SPAN, KEY_VALUE_HEADS, HEAD_SIZE)
        window_key_rows = apply_rotary(window_key_rows, slot_ids.astype(jnp.float32)).astype(jnp.bfloat16)
        window_value_rows = jnp.dot(window_row_inputs, value_projection, preferred_element_type=jnp.float32).astype(jnp.bfloat16).reshape(WINDOW_SPAN, KEY_VALUE_HEADS, HEAD_SIZE)
        grouped_query = query_for_row.astype(jnp.float32).reshape(KEY_VALUE_HEADS, heads_per_group, HEAD_SIZE)
        scores = jnp.einsum('kgd,wkd->kgw', grouped_query, window_key_rows.astype(jnp.float32)) * attention_scale
        fresh_score = jnp.einsum('kgd,kd->kg', grouped_query, row_key.astype(jnp.float32)) * attention_scale
        is_valid = slot_ids < row_length
        scores = jnp.where(is_valid[None, None, :], scores, -1e+30)
        row_max = jnp.maximum(lax.optimization_barrier(jnp.max(scores, axis=-1)), fresh_score)
        weights = jnp.where(is_valid[None, None, :], jnp.exp(scores - row_max[..., None]), 0.0)
        weight_new = jnp.exp(fresh_score - row_max)
        row_total = lax.optimization_barrier(jnp.sum(weights, axis=-1)) + weight_new
        weighted = jnp.einsum('kgw,wkd->kgd', weights, window_value_rows.astype(jnp.float32)) + weight_new[..., None] * row_value.astype(jnp.float32)[:, None, :]
        return (weighted / row_total[..., None]).reshape(QUERY_HEADS * HEAD_SIZE).astype(jnp.bfloat16)
    attended = lax.map(one_row, (cached_inputs, query, fresh_key, fresh_value, window_lengths))
    attn_term = jnp.dot(attended, w_attn_out, preferred_element_type=jnp.float32)
    hidden_out = (hidden_f + (ssm_term + mlp_term + attn_term)).astype(jnp.bfloat16)
    return (hidden_out, state_out)
```

```python
import jax
import jax.numpy as jnp
from jax import lax
from jax.sharding import PartitionSpec as P

HEAD_SIZE = 128


epsilon = 1e-05
rope_base = 10000.0


def apply_rotary(head_values, positions):
    half_dim = head_values.shape[-1] // 2
    frequency = rope_base ** (
        -(jnp.arange(half_dim, dtype=jnp.float32) * 2.0) / head_values.shape[-1]
    )
    angles = positions[..., None, None] * frequency
    cosine = jnp.cos(angles)
    sine_part = jnp.sin(angles)
    front_half = head_values[..., :half_dim]
    back_half = head_values[..., half_dim:]
    return jnp.concatenate(
        [front_half * cosine - back_half * sine_part, back_half * cosine + front_half * sine_part],
        axis=-1,
    )


BOTH = ("grp", "seq")


def gather_features(own):
    count = lax.axis_size(BOTH)
    rows = jnp.broadcast_to(own[None], (count,) + own.shape)
    blocks = lax.all_to_all(rows, BOTH, 0, 0)
    return blocks.transpose(1, 0, 2).reshape(own.shape[0], count * own.shape[1])


def exchange_sum(value):
    count = lax.axis_size(BOTH)
    step = 1
    while step < count:
        value = value + lax.ppermute(value, BOTH, [(i, i ^ step) for i in range(count)])
        step *= 2
    return value


def scatter_sum(term):
    count = lax.axis_size(BOTH)
    blocks = term.astype(jnp.bfloat16).reshape(term.shape[0], count, term.shape[1] // count)
    return jnp.sum(lax.all_to_all(blocks, BOTH, 1, 1).astype(jnp.float32), axis=1)


def per_device(
    hidden_in,
    norm_gain,
    w_ssm_in,
    w_ssm_gate,
    conv_weight,
    conv_bias,
    conv_state,
    w_state_proj,
    w_step,
    step_bias,
    log_decay,
    skip_gain,
    ssm_state,
    w_ssm_out,
    w_query,
    key_projection,
    value_projection,
    w_attn_out,
    w_mlp_gate,
    w_mlp_up,
    w_mlp_down,
    cached_inputs,
    window_lengths,
):
    batch_rows = hidden_in.shape[0]
    model_width = norm_gain.shape[0]
    hidden_f = hidden_in.astype(jnp.float32)
    raw_full = gather_features(hidden_in).astype(jnp.float32)
    row_scale = lax.rsqrt(jnp.mean(raw_full * raw_full, axis=1, keepdims=True) + epsilon)
    normed_input = (raw_full * row_scale * norm_gain).astype(jnp.bfloat16)
    ssm_input = jnp.dot(normed_input, w_ssm_in, preferred_element_type=jnp.float32).astype(
        jnp.bfloat16
    )
    gate_input = jnp.dot(normed_input, w_ssm_gate, preferred_element_type=jnp.float32)
    past_inputs = conv_state.astype(jnp.float32)
    conv_sum = (
        conv_bias
        + jnp.sum(past_inputs * conv_weight[:-1][None], axis=1)
        + conv_weight[-1] * lax.optimization_barrier(ssm_input).astype(jnp.float32)
    )
    conv_out = jax.nn.silu(conv_sum)
    rank_size = w_step.shape[0]
    state_size = log_decay.shape[0]
    low_rank = exchange_sum(
        jnp.dot(conv_out.astype(jnp.bfloat16), w_state_proj, preferred_element_type=jnp.float32)
    )
    step_low = low_rank[:, :rank_size].astype(jnp.bfloat16)
    input_map = low_rank[:, rank_size : rank_size + state_size]
    output_map = low_rank[:, rank_size + state_size :]
    step_size = jax.nn.softplus(
        jnp.dot(step_low, w_step, preferred_element_type=jnp.float32) + step_bias
    )
    decay_rate = jnp.exp(log_decay)
    state_out = (
        jnp.exp(-step_size[:, None, :] * decay_rate[None]) * ssm_state
        + step_size[:, None, :] * input_map[:, :, None] * conv_out[:, None, :]
    )
    ssm_mixed = jnp.sum(state_out * output_map[:, :, None], axis=1) + skip_gain * conv_out
    ssm_gated = (ssm_mixed * jax.nn.silu(gate_input)).astype(jnp.bfloat16)
    ssm_term = jnp.dot(ssm_gated, w_ssm_out, preferred_element_type=jnp.float32)
    gate_act = jnp.dot(normed_input, w_mlp_gate, preferred_element_type=jnp.float32)
    up_act = jnp.dot(normed_input, w_mlp_up, preferred_element_type=jnp.float32)
    mlp_hidden = (jax.nn.silu(gate_act) * up_act).astype(jnp.bfloat16)
    mlp_term = jnp.dot(mlp_hidden, w_mlp_down, preferred_element_type=jnp.float32)
    own_seqs = cached_inputs.shape[0]
    window_size = cached_inputs.shape[1]
    seq_start = lax.axis_index("seq") * own_seqs
    normed_own = lax.dynamic_slice_in_dim(normed_input, seq_start, own_seqs, 0)
    lengths_own = lax.dynamic_slice_in_dim(window_lengths, seq_start, own_seqs, 0)
    heads_here = w_query.shape[1] // HEAD_SIZE
    kv_here = key_projection.shape[1] // HEAD_SIZE
    heads_per_group = heads_here // kv_here
    attention_scale = HEAD_SIZE ** (-0.5)
    fresh_position = lengths_own.astype(jnp.float32)
    query = apply_rotary(
        jnp.dot(normed_own, w_query, preferred_element_type=jnp.float32).reshape(
            own_seqs, heads_here, HEAD_SIZE
        ),
        fresh_position,
    ).astype(jnp.bfloat16)
    fresh_key = apply_rotary(
        jnp.dot(normed_own, key_projection, preferred_element_type=jnp.float32).reshape(
            own_seqs, kv_here, HEAD_SIZE
        ),
        fresh_position,
    ).astype(jnp.bfloat16)
    fresh_value = (
        jnp.dot(normed_own, value_projection, preferred_element_type=jnp.float32)
        .astype(jnp.bfloat16)
        .reshape(own_seqs, kv_here, HEAD_SIZE)
    )
    flat_inputs = cached_inputs.reshape(own_seqs * window_size, model_width)
    slot_ids = jnp.arange(window_size, dtype=jnp.int32)
    positions = jnp.broadcast_to(slot_ids[None, :], (own_seqs, window_size)).astype(jnp.float32)
    window_key_rows = jnp.dot(
        flat_inputs, key_projection, preferred_element_type=jnp.float32
    ).reshape(own_seqs, window_size, kv_here, HEAD_SIZE)
    window_key_rows = apply_rotary(window_key_rows, positions).astype(jnp.bfloat16)
    window_value_rows = (
        jnp.dot(flat_inputs, value_projection, preferred_element_type=jnp.float32)
        .astype(jnp.bfloat16)
        .reshape(own_seqs, window_size, kv_here, HEAD_SIZE)
    )
    grouped_query = query.astype(jnp.float32).reshape(own_seqs, kv_here, heads_per_group, HEAD_SIZE)
    scores = (
        jnp.einsum("bkgd,bpkd->bkgp", grouped_query, window_key_rows.astype(jnp.float32))
        * attention_scale
    )
    fresh_score = (
        jnp.einsum("ynow,ynw->yno", grouped_query, fresh_key.astype(jnp.float32)) * attention_scale
    )
    is_valid = (slot_ids[None, :] < lengths_own[:, None])[:, None, None, :]
    scores = jnp.where(is_valid, scores, -1e30)
    joint_max = jnp.maximum(jnp.max(scores, axis=-1), fresh_score)
    weights = jnp.where(is_valid, jnp.exp(scores - joint_max[..., None]), 0.0)
    weight_new = jnp.exp(fresh_score - joint_max)
    joint_total = jnp.sum(weights, axis=-1) + weight_new
    joint_sum = (
        jnp.einsum("bkgp,bpkd->bkgd", weights, window_value_rows.astype(jnp.float32))
        + weight_new[..., None] * fresh_value.astype(jnp.float32)[:, :, None, :]
    )
    attended_own = (
        (joint_sum / joint_total[..., None])
        .reshape(own_seqs, heads_here * HEAD_SIZE)
        .astype(jnp.bfloat16)
    )
    seq_count = lax.axis_size("seq")
    attended = lax.all_to_all(
        jnp.broadcast_to(attended_own[None], (seq_count,) + attended_own.shape), "seq", 0, 0
    ).reshape(batch_rows, heads_here * HEAD_SIZE)
    attn_cols = jnp.dot(attended, w_attn_out, preferred_element_type=jnp.float32)
    col_start = lax.axis_index("seq") * w_attn_out.shape[1]
    attn_term = lax.dynamic_update_slice(
        jnp.zeros((batch_rows, model_width), jnp.float32), attn_cols, (jnp.int32(0), col_start)
    )
    summed = scatter_sum(mlp_term + attn_term + ssm_term)
    hidden_out = (hidden_f + summed).astype(jnp.bfloat16)
    return (hidden_out, state_out)


def solution(mesh):
    placed = (
        P(None, ("grp", "seq")),
        P(),
        P(None, ("grp", "seq")),
        P(None, ("grp", "seq")),
        P(None, ("grp", "seq")),
        P(("grp", "seq")),
        P(None, None, ("grp", "seq")),
        P(("grp", "seq"), None),
        P(None, ("grp", "seq")),
        P(("grp", "seq")),
        P(None, ("grp", "seq")),
        P(("grp", "seq")),
        P(None, None, ("grp", "seq")),
        P(("grp", "seq"), None),
        P(None, "grp"),
        P(None, "grp"),
        P(None, "grp"),
        P("grp", "seq"),
        P(None, ("grp", "seq")),
        P(None, ("grp", "seq")),
        P(("grp", "seq"), None),
        P("seq", None, None),
        P(),
    )
    return jax.shard_map(
        per_device,
        mesh=mesh,
        in_specs=placed,
        out_specs=(P(None, ("grp", "seq")), P(None, None, ("grp", "seq"))),
        check_vma=False,
    )
```

```python
import functools

import jax
import jax.numpy as jnp
import numpy as np
from jax import lax
from jax.experimental import pallas as pl
from jax.experimental.pallas import tpu as pltpu
from jax.sharding import PartitionSpec as P

HEAD_SIZE = 128
BOTH = ("grp", "seq")
F32 = jnp.float32
BF16 = jnp.bfloat16

epsilon = 1e-05
rope_base = 10000.0


def rope_frequency():
    half = HEAD_SIZE // 2
    return rope_base ** (-(np.arange(half, dtype=np.float64) * 2.0) / HEAD_SIZE)


def rope_tables(count):
    angles = np.arange(count, dtype=np.float64)[:, None] * rope_frequency()[None]
    cosine, sine = np.cos(angles), np.sin(angles)
    return (
        np.concatenate([cosine, cosine], 1).astype(np.float32),
        np.concatenate([-sine, sine], 1).astype(np.float32),
    )


def rotate(head, cosine, sine):
    return head * cosine + pltpu.roll(head, HEAD_SIZE // 2, 1) * sine


def lanes(h):
    return slice(h * HEAD_SIZE, (h + 1) * HEAD_SIZE)


VMEM_SPEC = pl.BlockSpec(memory_space=pltpu.VMEM)
HBM_SPEC = pl.BlockSpec(memory_space=pltpu.HBM)
SMEM_SPEC = pl.BlockSpec(memory_space=pltpu.SMEM)


def call(body, name, vmem_mib, flops, moved, **kwargs):
    return pl.pallas_call(
        body,
        name=name,
        compiler_params=pltpu.CompilerParams(vmem_limit_bytes=vmem_mib << 20),
        cost_estimate=pl.CostEstimate(flops=int(flops), transcendentals=0, bytes_accessed=int(moved)),
        **kwargs,
    )


def in_hbm(array):
    return pltpu.with_memory_space_constraint(array, pltpu.HBM)


def dot(a, b):
    return jnp.dot(a, b, preferred_element_type=F32)


def dot_t(a, b):
    return lax.dot_general(a, b, (((1,), (1,)), ((), ())), preferred_element_type=F32)


class Loads:
    def __init__(self, groups, depth, most=None):
        self.groups, self.started = groups, 0
        self.ahead = (most or depth) - depth
        for _ in range(depth):
            self.start_next()

    def start_next(self):
        if self.started < len(self.groups):
            for copy in self.groups[self.started]:
                copy.start()
            self.started += 1

    def wait(self, n):
        for copy in self.groups[n]:
            copy.wait()
        self.start_next()
        if self.ahead > 0:
            self.ahead -= 1
            self.start_next()


def pieces_of(size, most, step=16):
    while size % most or (size // most) % step:
        most //= 2
    return most


def silu(v):
    return v / (1.0 + jnp.exp(-v))


def nbytes(*arrays):
    return sum(a.size * a.dtype.itemsize for a in arrays)


def window_body(
    x_hbm, wk_hbm, wv_hbm, cos_hbm, sin_hbm, wi_hbm,
    k_ref, v_hbm, wi,
    x, wkv, total, v_ref, cos_ref, sin_ref, xsem, ksem, vsem, rsem, isem, tsem, osem, *, seqs, chunks, sub,
):
    rows = total.shape[0]
    width = x.shape[1]
    cols = wk_hbm.shape[1]
    size = width // chunks
    groups = []
    for c in range(chunks):
        at = pl.ds(c * size, size)
        groups.append(
            [
                pltpu.make_async_copy(x_hbm.at[pl.ds(0, rows), at], x.at[pl.ds(0, rows), at], xsem.at[c]),
                pltpu.make_async_copy(wk_hbm.at[at], wkv.at[at, pl.ds(0, cols)], ksem.at[c]),
                pltpu.make_async_copy(wv_hbm.at[at], wkv.at[at, pl.ds(cols, cols)], vsem.at[c]),
            ]
        )
    groups[1] += [
        pltpu.make_async_copy(cos_hbm, cos_ref, tsem.at[0]),
        pltpu.make_async_copy(sin_hbm, sin_ref, tsem.at[1]),
    ]
    part = rows // sub
    for n in range((seqs - 1) * sub):
        at = pl.ds(rows + n * part, part)
        groups.append([pltpu.make_async_copy(x_hbm.at[at], x.at[at], rsem.at[n])])
    groups.append([pltpu.make_async_copy(wi_hbm, wi, isem)])
    loads = Loads(groups, *WINDOW_DEPTH)

    def finish(b, kv):
        at = slice(b * rows, (b + 1) * rows)
        for h in range(cols // HEAD_SIZE):
            turned = rotate(kv[:, lanes(h)], cos_ref[:rows, :], sin_ref[:rows, :])
            k_ref[at, lanes(h)] = turned.astype(BF16)
        v_ref[at, :] = kv[:, cols:].astype(BF16)
        store = pltpu.make_async_copy(v_ref.at[at], v_hbm.at[at], osem.at[b])
        store.start()
        return store

    for c in range(chunks):
        loads.wait(c)
        at = slice(c * size, (c + 1) * size)
        term = dot(x[:rows, at], wkv[at, :])
        if c == 0:
            total[...] = term
        else:
            total[...] += term
    stores = [finish(0, total[...])]
    for b in range(1, seqs):
        for n in range(sub):
            loads.wait(chunks + (b - 1) * sub + n)
        stores.append(finish(b, dot(x[b * rows : (b + 1) * rows, :], wkv[...])))
    loads.wait(len(groups) - 1)
    for store in stores:
        store.wait()


WINDOW_DEPTH = (6, 6)
WINDOW_CUTS = (4, 2)


def window_stage(cached, wk, wv, wi, cosine, sine):
    seqs, window, width = cached.shape
    cols = wk.shape[1]
    chunks, sub = WINDOW_CUTS
    flat = cached.reshape(seqs * window, width)
    out = jax.ShapeDtypeStruct((seqs * window, cols), BF16)
    sems = pltpu.SemaphoreType.DMA
    return call(
        functools.partial(window_body, seqs=seqs, chunks=chunks, sub=sub),
        "window",
        30,
        4 * cached.size * cols,
        nbytes(cached, wk, wv, wi),
        out_shape=(out, pltpu.HBM(out.shape, BF16), jax.ShapeDtypeStruct(wi.shape, BF16)),
        in_specs=[HBM_SPEC] * 6,
        out_specs=(VMEM_SPEC, HBM_SPEC, VMEM_SPEC),
        scratch_shapes=[
            pltpu.VMEM(flat.shape, BF16),
            pltpu.VMEM((width, 2 * cols), BF16),
            pltpu.VMEM((window, 2 * cols), F32),
            pltpu.VMEM(out.shape, BF16),
            pltpu.VMEM(cosine.shape, F32),
            pltpu.VMEM(sine.shape, F32),
            sems((chunks,)),
            sems((chunks,)),
            sems((chunks,)),
            sems(((seqs - 1) * sub,)),
            sems,
            sems((2,)),
            sems((seqs,)),
        ],
    )(*map(in_hbm, (flat, wk, wv, cosine, sine, wi)))


def head_body(
    x_ref, gain_ref, tap_ref, bias_ref, past_ref, wi_ref, ws_ref, normed_ref, conv_ref, low_ref, xf
):
    count, _, part = x_ref.shape
    for n in range(count):
        xf[:, n * part : (n + 1) * part] = x_ref[n].astype(F32)
    x = xf[...]
    scale = lax.rsqrt(jnp.sum(x * x, axis=1, keepdims=True) / x.shape[1] + epsilon)
    normed = (x * scale * gain_ref[...]).astype(BF16)
    normed_ref[...] = normed
    ssm_input = dot(normed, wi_ref[...]).astype(BF16).astype(F32)
    taps = past_ref.shape[0]
    summed = bias_ref[...]
    for t in range(taps):
        summed = summed + past_ref[t].astype(F32) * tap_ref[t : t + 1, :]
    conv = silu(summed + tap_ref[taps : taps + 1, :] * ssm_input)
    conv_ref[...] = conv
    low_ref[...] = dot_t(conv.astype(BF16), ws_ref[...])


def head_stage(blocks, gain, taps, bias, past, w_in, w_state):
    count, rows, part = blocks.shape
    width, cols = w_in.shape
    if part % 128:
        blocks = blocks.transpose(1, 0, 2).reshape(1, rows, width)
    return call(
        head_body,
        "head",
        16,
        2 * rows * w_in.size,
        nbytes(w_in, w_state),
        out_shape=(
            jax.ShapeDtypeStruct((rows, width), BF16),
            jax.ShapeDtypeStruct((rows, cols), F32),
            jax.ShapeDtypeStruct((rows, w_state.shape[1]), F32),
        ),
        in_specs=[VMEM_SPEC] * 7,
        out_specs=(VMEM_SPEC,) * 3,
        scratch_shapes=[pltpu.VMEM((rows, width), F32)],
    )(blocks, gain[None], taps, bias[None], past.transpose(1, 0, 2), w_in, w_state.T)


def attention_body(
    len_ref, x_ref, wk_hbm, wv_hbm, wq_hbm, v_hbm, cos_hbm, sin_hbm, k_ref, out_ref,
    wk, wv, wq, v_ref, cos_near, sin_near, k_all, v_all, q_all, ksem, vsem, qsem, csem, nsem, *, seqs,
):
    start = lax.axis_index("seq") * seqs
    near = []
    for b in range(seqs):
        at = pl.ds(pl.multiple_of(len_ref[start + b] // 8 * 8, 8), 8)
        near.append(pltpu.make_async_copy(cos_hbm.at[at], cos_near.at[b], nsem.at[b]))
        near.append(pltpu.make_async_copy(sin_hbm.at[at], sin_near.at[b], nsem.at[seqs + b]))
    for copy in near:
        copy.start()
    pieces = ksem.shape[0]
    size = wk.shape[0] // pieces
    at = [pl.ds(c * size, size) for c in range(pieces)]
    groups = [
        [
            pltpu.make_async_copy(wk_hbm.at[at[c]], wk.at[at[c]], ksem.at[c]),
            pltpu.make_async_copy(wv_hbm.at[at[c]], wv.at[at[c]], vsem.at[c]),
        ]
        for c in range(pieces)
    ]
    groups += [[pltpu.make_async_copy(wq_hbm.at[at[c]], wq.at[at[c]], qsem.at[c])] for c in range(pieces)]
    groups.append([pltpu.make_async_copy(v_hbm, v_ref, csem)])
    loads = Loads(groups, 5)
    for c in range(pieces):
        loads.wait(c)
        x = x_ref[:, c * size : (c + 1) * size]
        for total, w in ((k_all, wk), (v_all, wv)):
            term = dot(x, w[at[c], :])
            total[...] = term if c == 0 else total[...] + term
    for c in range(pieces):
        loads.wait(pieces + c)
        term = dot(x_ref[:, c * size : (c + 1) * size], wq[at[c], :])
        q_all[...] = term if c == 0 else q_all[...] + term
    heads = q_all.shape[1] // HEAD_SIZE
    kv = k_all.shape[1] // HEAD_SIZE
    group = heads // kv
    window = k_ref.shape[0] // seqs
    for copy in near:
        copy.wait()
    fresh_row = lambda ref: jnp.concatenate(
        [ref[b, pl.ds(len_ref[start + b] % 8, 1), :] for b in range(seqs)], 0
    )
    cosine, sine = fresh_row(cos_near), fresh_row(sin_near)
    pick = lambda ref: jnp.concatenate([ref[pl.ds(start + b, 1), :] for b in range(seqs)], 0)
    q_own, k_own, v_own = pick(q_all), pick(k_all), pick(v_all)
    q = [rotate(q_own[:, lanes(h)], cosine, sine) for h in range(heads)]
    fresh = [rotate(k_own[:, lanes(j)], cosine, sine) for j in range(kv)]
    fresh_k = jnp.concatenate(fresh, 1).astype(BF16).astype(F32)
    fresh_v = v_own.astype(BF16).astype(F32)
    zero = jnp.zeros((1, HEAD_SIZE), F32)
    scale = HEAD_SIZE ** (-0.5)
    loads.wait(2 * pieces)
    for b in range(seqs):
        rows = [
            jnp.concatenate([q[h][b : b + 1] if j == h // group else zero for j in range(kv)], 1)
            for h in range(heads)
        ]
        q_b = jnp.concatenate(rows, 0).astype(BF16)
        v_b = v_ref[b * window : (b + 1) * window, :]
        scores = dot_t(q_b, k_ref[b * window : (b + 1) * window, :]) * scale
        fresh_score = jnp.sum(q_b.astype(F32) * fresh_k[b : b + 1], axis=1, keepdims=True) * scale
        valid = lax.broadcasted_iota(jnp.int32, scores.shape, 1) < len_ref[start + b]
        scores = jnp.where(valid, scores, -1e30)
        top = jnp.maximum(jnp.max(scores, axis=1, keepdims=True), fresh_score)
        weights = jnp.where(valid, jnp.exp(scores - top), 0.0)
        weight_new = jnp.exp(fresh_score - top)
        total = jnp.sum(weights, axis=1, keepdims=True) + weight_new
        coarse = weights.astype(BF16)
        fine = (weights - coarse.astype(F32)).astype(BF16)
        mixed = (dot(coarse, v_b) + dot(fine, v_b) + weight_new * fresh_v[b : b + 1]) / total
        for h in range(heads):
            out_ref[h * seqs + b : h * seqs + b + 1, :] = mixed[h : h + 1, lanes(h // group)]


def attention_stage(lengths, normed, wq, wk, wv, keys, values, cosine, sine):
    seqs = lengths.shape[0] // lax.axis_size("seq")
    rows = normed.shape[0]
    pieces = 4
    sems = pltpu.SemaphoreType.DMA
    return call(
        functools.partial(attention_body, seqs=seqs),
        "attention",
        16,
        2 * rows * (wq.size + wk.size + wv.size) + 8 * keys.size,
        nbytes(wq, wk, wv, keys, values),
        out_shape=jax.ShapeDtypeStruct((seqs * wq.shape[1] // HEAD_SIZE, HEAD_SIZE), F32),
        in_specs=[SMEM_SPEC, VMEM_SPEC] + [HBM_SPEC] * 6 + [VMEM_SPEC],
        out_specs=VMEM_SPEC,
        scratch_shapes=[
            pltpu.VMEM(wk.shape, BF16),
            pltpu.VMEM(wv.shape, BF16),
            pltpu.VMEM(wq.shape, BF16),
            pltpu.VMEM(values.shape, BF16),
            pltpu.VMEM((seqs, 8, HEAD_SIZE), F32),
            pltpu.VMEM((seqs, 8, HEAD_SIZE), F32),
            pltpu.VMEM((rows, wk.shape[1]), F32),
            pltpu.VMEM((rows, wv.shape[1]), F32),
            pltpu.VMEM((rows, wq.shape[1]), F32),
            sems((pieces,)),
            sems((pieces,)),
            sems((pieces,)),
            sems,
            sems((2 * seqs,)),
        ],
    )(in_hbm(lengths), normed, *map(in_hbm, (wk, wv, wq, values, cosine, sine)), keys)


def pack_body(*refs):
    parts = [ref[...] for ref in refs[:-3]]
    attended_ref, out_ref, buf = refs[-3:]
    while len(parts) > 1:
        parts = [sum(parts[n : n + 2]) for n in range(0, len(parts), 2)]
    total = parts[0]
    batch, width = total.shape
    heads = attended_ref.shape[0]
    coarse = total.astype(BF16).astype(F32)
    buf[...] = jnp.zeros_like(buf)
    buf[:batch, :width] = coarse
    buf[batch : 2 * batch, :width] = total - coarse
    buf[2 * batch : 2 * batch + heads, :HEAD_SIZE] = attended_ref[...]
    out_ref[...] = jnp.broadcast_to(buf[...].astype(BF16)[None], out_ref.shape)


def pack_stage(parts, attended, count):
    batch, width = parts[0].shape
    rows = -(-(2 * batch + attended.shape[0]) // 16) * 16
    cols = -(-width // 128) * 128
    return call(
        pack_body,
        "pack",
        16,
        parts[0].size,
        nbytes(*parts),
        out_shape=jax.ShapeDtypeStruct((count, rows, cols), BF16),
        in_specs=[VMEM_SPEC] * (len(parts) + 1),
        out_specs=VMEM_SPEC,
        scratch_shapes=[pltpu.VMEM((rows, cols), F32)],
    )(*parts, attended)


def mlp_body(
    x_ref, ws_hbm, wg_hbm, wu_hbm, wd_hbm, wo_hbm, st_hbm, state_hbm, skip_hbm, bias_hbm, decay_hbm, conv_ref,
    gain_ref, direct_ref, aux_ref, out_ref, wo, st, state,
    ws, wg, wu, wd, skip_ref, bias_ref, decay_ref, g_all, u_all, ssem, gsem, usem, dsem, osem,
):
    small = [
        pltpu.make_async_copy(skip_hbm, skip_ref, osem.at[3]),
        pltpu.make_async_copy(bias_hbm, bias_ref, osem.at[4]),
        pltpu.make_async_copy(decay_hbm, decay_ref, osem.at[5]),
    ]
    for copy in small:
        copy.start()
    width = x_ref.shape[1]
    inner = wg.shape[0]
    pieces = gsem.shape[0]
    chunks = dsem.shape[0]
    size = width // chunks
    part = inner // pieces
    cut = lambda n, step: pl.ds(n * step, step)
    groups = [
        [pltpu.make_async_copy(ws_hbm.at[cut(c, size)], ws.at[cut(c, size)], ssem.at[c])] for c in range(chunks)
    ]
    groups += [
        [
            pltpu.make_async_copy(wg_hbm.at[cut(n, part)], wg.at[cut(n, part)], gsem.at[n]),
            pltpu.make_async_copy(wu_hbm.at[cut(n, part)], wu.at[cut(n, part)], usem.at[n]),
        ]
        for n in range(pieces)
    ]
    groups += [
        [pltpu.make_async_copy(wd_hbm.at[:, cut(c, size)], wd.at[:, cut(c, size)], dsem.at[c])]
        for c in range(chunks)
    ]
    groups.append([pltpu.make_async_copy(state_hbm, state, osem.at[0])])
    groups.append([pltpu.make_async_copy(st_hbm, st, osem.at[1])])
    groups.append([pltpu.make_async_copy(wo_hbm.at[pl.ds(0, wo.shape[0])], wo, osem.at[2])])
    loads = Loads(groups, 6)
    gate = None
    for c in range(chunks):
        loads.wait(c)
        term = dot(x_ref[:, cut(c, size)], ws[cut(c, size), :])
        gate = term if gate is None else gate + term
    gain_ref[...] = silu(gate)
    for copy in small:
        copy.wait()
    states = decay_ref.shape[0]
    aux_ref[:states, :] = jnp.exp(decay_ref[...])
    aux_ref[states:, :] = jnp.broadcast_to(bias_ref[...], (8, bias_ref.shape[1]))
    direct_ref[...] = skip_ref[...] * conv_ref[...]
    x = x_ref[...]
    for n in range(pieces):
        loads.wait(chunks + n)
        g_all[cut(n, part), :] = dot_t(wg[cut(n, part), :], x)
        u_all[cut(n, part), :] = dot_t(wu[cut(n, part), :], x)
    hidden = (silu(g_all[...]) * u_all[...]).T.astype(BF16)
    for c in range(chunks):
        loads.wait(chunks + pieces + c)
        out_ref[:, cut(c, size)] = dot(hidden, wd[:, cut(c, size)])
    for n in range(3):
        loads.wait(2 * chunks + pieces + n)


def mlp_stage(normed, ws, wg, wu, wd, wo, st, state, conv, skip, bias, decay):
    rows, width = normed.shape
    wg, wu = wg.T, wu.T
    inner, cols = wg.shape[0], ws.shape[1]
    pieces, chunks = pieces_of(inner, 4), 4
    like = lambda a: jax.ShapeDtypeStruct(a.shape, a.dtype)
    sems = pltpu.SemaphoreType.DMA
    return call(
        mlp_body,
        "mlp",
        24,
        2 * rows * (ws.size + wg.size + wu.size + wd.size),
        nbytes(ws, wg, wu, wd, wo),
        out_shape=(
            like(conv),
            like(conv),
            jax.ShapeDtypeStruct((decay.shape[0] + 8, cols), F32),
            jax.ShapeDtypeStruct((rows, width), F32),
            jax.ShapeDtypeStruct((wo.shape[0] // 2, width), BF16),
            like(st),
            like(state),
        ),
        in_specs=[VMEM_SPEC] + [HBM_SPEC] * 10 + [VMEM_SPEC],
        out_specs=(VMEM_SPEC,) * 7,
        scratch_shapes=[
            pltpu.VMEM(ws.shape, BF16),
            pltpu.VMEM(wg.shape, BF16),
            pltpu.VMEM(wu.shape, BF16),
            pltpu.VMEM(wd.shape, BF16),
            pltpu.VMEM((1, cols), F32),
            pltpu.VMEM((1, cols), F32),
            pltpu.VMEM(decay.shape, F32),
            pltpu.VMEM((inner, rows), F32),
            pltpu.VMEM((inner, rows), F32),
            sems((chunks,)),
            sems((pieces,)),
            sems((pieces,)),
            sems((chunks,)),
            sems((6,)),
        ],
    )(normed, *map(in_hbm, (ws, wg, wu, wd, wo, st, state, skip[None], bias[None], decay)), conv)


def tail_body(
    pack_ref, aux_ref, conv_ref, gain_ref, direct_ref, other_ref, st_ref, state, wo_ref, wo_hbm, wa_hbm,
    state_out, term_ref, total, rows_f, wo, wa, sems, *, seqs, heads,
):
    half = wo.shape[0]
    loads = [
        pltpu.make_async_copy(wo_hbm.at[pl.ds(half, half)], wo, sems.at[0]),
        pltpu.make_async_copy(wa_hbm, wa, sems.at[1]),
    ]
    for copy in loads:
        copy.start()
    rank = st_ref.shape[0]
    states = aux_ref.shape[0] - 8
    batch = conv_ref.shape[0]
    groups = pack_ref.shape[0]
    low = jnp.zeros((batch, rank + 2 * states), F32)
    for n in range(groups):
        rows = pack_ref[n].astype(F32)
        low += rows[:batch, : rank + 2 * states] + rows[batch : 2 * batch, : rank + 2 * states]
        for h in range(heads):
            at = 2 * batch + h * seqs
            rows_f[n * seqs : (n + 1) * seqs, lanes(h)] = rows[at : at + seqs, :HEAD_SIZE]
    maps = low[:, rank:].T
    raw = dot(low[:, :rank].astype(BF16), st_ref[...]) + aux_ref[states : states + 1, :]
    step = jnp.maximum(raw, 0.0) + jnp.log1p(jnp.exp(-jnp.abs(raw)))
    rate = aux_ref[:states, :]
    drive = step * conv_ref[...]
    mixed = []
    for b in range(batch):
        kept = jnp.exp(-step[b : b + 1] * rate) * state[b]
        new = kept + drive[b : b + 1] * maps[:states, b : b + 1]
        state_out[b] = new
        mixed.append(jnp.sum(new * maps[states:, b : b + 1], axis=0, keepdims=True))
    gated = (jnp.concatenate(mixed, 0) + direct_ref[...]) * gain_ref[...]
    gated = gated.astype(BF16)
    total[...] = other_ref[...] + dot(gated[:, :half], wo_ref[...])
    loads[0].wait()
    total[...] += dot(gated[:, half:], wo[...])
    loads[1].wait()
    cols = wa.shape[1]
    at = pl.ds(pl.multiple_of(lax.axis_index("seq") * cols, cols), cols)
    total[:, at] += dot(rows_f[...].astype(BF16), wa[...])
    count, _, part = term_ref.shape
    for n in range(count):
        term_ref[n] = total[:, n * part : (n + 1) * part].astype(BF16)


def tail_stage(packed, aux, conv, gain, direct, other, st, state, wo, w_out, wa, count):
    rows, width = other.shape
    seqs = rows // packed.shape[0]
    inner = wa.shape[0]
    sent, part = count, width // count
    if part % 128:
        sent, part = 1, width
    return call(
        functools.partial(tail_body, seqs=seqs, heads=inner // HEAD_SIZE),
        "tail",
        16,
        2 * rows * wo.size,
        nbytes(wo, state, state),
        out_shape=(
            jax.ShapeDtypeStruct(state.shape, F32),
            jax.ShapeDtypeStruct((sent, rows, part), BF16),
        ),
        in_specs=[VMEM_SPEC] * 9 + [HBM_SPEC] * 2,
        out_specs=(VMEM_SPEC, VMEM_SPEC),
        scratch_shapes=[
            pltpu.VMEM((rows, width), F32),
            pltpu.VMEM((rows, inner), F32),
            pltpu.VMEM(wo.shape, BF16),
            pltpu.VMEM(wa.shape, BF16),
            pltpu.SemaphoreType.DMA((2,)),
        ],
    )(packed, aux, conv, gain, direct, other, st, state, wo, in_hbm(w_out), in_hbm(wa))


def spread_body(x_ref, out_ref):
    out_ref[...] = jnp.broadcast_to(x_ref[...][None], out_ref.shape)


def spread_stage(own, count):
    return call(
        spread_body, "spread", 4, 0, 0,
        out_shape=jax.ShapeDtypeStruct((count,) + own.shape, own.dtype),
    )(own)


def close_body(own_ref, blocks_ref, out_ref):
    total = own_ref[...].astype(F32)
    parts = [blocks_ref[n].astype(F32) for n in range(blocks_ref.shape[0])]
    while len(parts) > 1:
        parts = [sum(parts[n : n + 2]) for n in range(0, len(parts), 2)]
    out_ref[...] = (total + parts[0]).astype(out_ref.dtype)


def close_stage(own, blocks):
    return call(
        close_body, "close", 4, blocks.size, 0,
        out_shape=jax.ShapeDtypeStruct(own.shape, own.dtype),
    )(own, blocks)


def gather_blocks(own):
    return lax.all_to_all(spread_stage(own, lax.axis_size(BOTH)), BOTH, 0, 0)


def exchange(value, axis, step):
    return lax.ppermute(value, axis, [(i, i ^ step) for i in range(lax.axis_size(axis))])


def per_device(
    hidden_in,
    norm_gain,
    w_ssm_in,
    w_ssm_gate,
    conv_weight,
    conv_bias,
    conv_state,
    w_state_proj,
    w_step,
    step_bias,
    log_decay,
    skip_gain,
    ssm_state,
    w_ssm_out,
    w_query,
    key_projection,
    value_projection,
    w_attn_out,
    w_mlp_gate,
    w_mlp_up,
    w_mlp_down,
    cached_inputs,
    window_lengths,
):
    batch_rows = hidden_in.shape[0]
    count = lax.axis_size(BOTH)
    blocks = gather_blocks(hidden_in)
    cosine, sine = map(jnp.asarray, rope_tables(cached_inputs.shape[1] + 8))
    keys, values, wi = window_stage(cached_inputs, key_projection, value_projection, w_ssm_in, cosine, sine)
    blocks, keys = lax.optimization_barrier((blocks, keys))
    normed, conv_out, low_part = head_stage(
        blocks, norm_gain, conv_weight, conv_bias, conv_state, wi, w_state_proj
    )
    low_parts = [low_part] + [exchange(low_part, "grp", n) for n in range(1, lax.axis_size("grp"))]
    attended = attention_stage(
        window_lengths, normed, w_query, key_projection, value_projection, keys, values, cosine, sine
    )
    packed = pack_stage(low_parts, attended, lax.axis_size("seq"))
    packed, normed = lax.optimization_barrier((packed, normed))
    received = lax.all_to_all(packed, "seq", 0, 0)
    gain, direct, aux, other, wo, st, state = mlp_stage(
        normed, w_ssm_gate, w_mlp_gate, w_mlp_up, w_mlp_down, w_ssm_out, w_step, ssm_state,
        conv_out, skip_gain, step_bias, log_decay,
    )
    state_out, terms = tail_stage(
        received, aux, conv_out, gain, direct, other, st, state, wo, w_ssm_out, w_attn_out, count
    )
    if terms.shape[0] != count:
        terms = terms.reshape(batch_rows, count, -1).transpose(1, 0, 2)
    hidden_out = close_stage(hidden_in, lax.all_to_all(terms, BOTH, 0, 0))
    return (hidden_out, state_out)


def solution(mesh):
    placed = (
        P(None, ("grp", "seq")),
        P(),
        P(None, ("grp", "seq")),
        P(None, ("grp", "seq")),
        P(None, ("grp", "seq")),
        P(("grp", "seq")),
        P(None, None, ("grp", "seq")),
        P(("grp", "seq"), None),
        P(None, ("grp", "seq")),
        P(("grp", "seq")),
        P(None, ("grp", "seq")),
        P(("grp", "seq")),
        P(None, None, ("grp", "seq")),
        P(("grp", "seq"), None),
        P(None, "grp"),
        P(None, "grp"),
        P(None, "grp"),
        P("grp", "seq"),
        P(None, ("grp", "seq")),
        P(None, ("grp", "seq")),
        P(("grp", "seq"), None),
        P("seq", None, None),
        P(),
    )
    return jax.shard_map(
        per_device,
        mesh=mesh,
        in_specs=placed,
        out_specs=(P(None, ("grp", "seq")), P(None, None, ("grp", "seq"))),
        check_vma=False,
    )
```

```python
import functools

import jax
import jax.numpy as jnp
import numpy as np
from jax import lax
from jax.experimental import pallas as pl
from jax.experimental.pallas import tpu as pltpu
from jax.sharding import PartitionSpec as P

HEAD_SIZE = 128
BOTH = ("grp", "seq")
F32 = jnp.float32
BF16 = jnp.bfloat16

epsilon = 1e-05
rope_base = 10000.0


def rope_frequency():
    half = HEAD_SIZE // 2
    return rope_base ** (-(np.arange(half, dtype=np.float64) * 2.0) / HEAD_SIZE)


def rope_tables(count):
    angles = np.arange(count, dtype=np.float64)[:, None] * rope_frequency()[None]
    cosine, sine = np.cos(angles), np.sin(angles)
    return (
        np.concatenate([cosine, cosine], 1).astype(np.float32),
        np.concatenate([-sine, sine], 1).astype(np.float32),
    )


def rotate(head, cosine, sine):
    return head * cosine + pltpu.roll(head, HEAD_SIZE // 2, 1) * sine


def lanes(h):
    return slice(h * HEAD_SIZE, (h + 1) * HEAD_SIZE)


VMEM_SPEC = pl.BlockSpec(memory_space=pltpu.VMEM)
HBM_SPEC = pl.BlockSpec(memory_space=pltpu.HBM)
SMEM_SPEC = pl.BlockSpec(memory_space=pltpu.SMEM)


def call(body, name, vmem_mib, flops, moved, **kwargs):
    return pl.pallas_call(
        body,
        name=name,
        compiler_params=pltpu.CompilerParams(vmem_limit_bytes=vmem_mib << 20),
        cost_estimate=pl.CostEstimate(flops=int(flops), transcendentals=0, bytes_accessed=int(moved)),
        **kwargs,
    )


def in_hbm(array):
    return pltpu.with_memory_space_constraint(array, pltpu.HBM)


def dot(a, b):
    return jnp.dot(a, b, preferred_element_type=F32)


def dot_t(a, b):
    return lax.dot_general(a, b, (((1,), (1,)), ((), ())), preferred_element_type=F32)


class Loads:
    def __init__(self, groups, depth, most=None):
        self.groups, self.started = groups, 0
        self.ahead = (most or depth) - depth
        for _ in range(depth):
            self.start_next()

    def start_next(self):
        if self.started < len(self.groups):
            for copy in self.groups[self.started]:
                copy.start()
            self.started += 1

    def wait(self, n):
        for copy in self.groups[n]:
            copy.wait()
        self.start_next()
        if self.ahead > 0:
            self.ahead -= 1
            self.start_next()


def pieces_of(size, most, step=16):
    while size % most or (size // most) % step:
        most //= 2
    return most


def silu(v):
    return v / (1.0 + jnp.exp(-v))


def nbytes(*arrays):
    return sum(a.size * a.dtype.itemsize for a in arrays)


def window_body(
    x_hbm, wk_hbm, wv_hbm, cos_hbm, sin_hbm, wi_hbm,
    k_ref, v_hbm, wi,
    x, wk, wv, k_sum, v_sum, v_ref, cos_ref, sin_ref, xsem, ksem, vsem, rsem, isem, tsem, osem, *, seqs, chunks, sub,
):
    rows = k_sum.shape[0]
    width = x.shape[1]
    size = width // chunks
    groups = []
    for c in range(chunks):
        at = pl.ds(c * size, size)
        groups.append(
            [
                pltpu.make_async_copy(x_hbm.at[pl.ds(0, rows), at], x.at[pl.ds(0, rows), at], xsem.at[c]),
                pltpu.make_async_copy(wk_hbm.at[at], wk.at[at], ksem.at[c]),
                pltpu.make_async_copy(wv_hbm.at[at], wv.at[at], vsem.at[c]),
            ]
        )
    groups[1] += [
        pltpu.make_async_copy(cos_hbm, cos_ref, tsem.at[0]),
        pltpu.make_async_copy(sin_hbm, sin_ref, tsem.at[1]),
    ]
    part = rows // sub
    for n in range((seqs - 1) * sub):
        at = pl.ds(rows + n * part, part)
        groups.append([pltpu.make_async_copy(x_hbm.at[at], x.at[at], rsem.at[n])])
    groups.append([pltpu.make_async_copy(wi_hbm, wi, isem)])
    loads = Loads(groups, *WINDOW_DEPTH)

    def finish(b, k, v):
        at = slice(b * rows, (b + 1) * rows)
        for h in range(k.shape[1] // HEAD_SIZE):
            turned = rotate(k[:, lanes(h)], cos_ref[:rows, :], sin_ref[:rows, :])
            k_ref[at, lanes(h)] = turned.astype(BF16)
        v_ref[at, :] = v.astype(BF16)
        store = pltpu.make_async_copy(v_ref.at[at], v_hbm.at[at], osem.at[b])
        store.start()
        return store

    for c in range(chunks):
        loads.wait(c)
        at = slice(c * size, (c + 1) * size)
        for total, w in ((k_sum, wk), (v_sum, wv)):
            term = dot(x[:rows, at], w[at, :])
            total[...] = term if c == 0 else total[...] + term
    stores = [finish(0, k_sum[...], v_sum[...])]
    for b in range(1, seqs):
        for n in range(sub):
            loads.wait(chunks + (b - 1) * sub + n)
        own = x[b * rows : (b + 1) * rows, :]
        stores.append(finish(b, dot(own, wk[...]), dot(own, wv[...])))
    loads.wait(len(groups) - 1)
    for store in stores:
        store.wait()


WINDOW_DEPTH = (4, 5)
WINDOW_CUTS = (4, 2)


def window_stage(cached, wk, wv, wi, cosine, sine):
    seqs, window, width = cached.shape
    cols = wk.shape[1]
    chunks, sub = WINDOW_CUTS
    flat = cached.reshape(seqs * window, width)
    out = jax.ShapeDtypeStruct((seqs * window, cols), BF16)
    sems = pltpu.SemaphoreType.DMA
    return call(
        functools.partial(window_body, seqs=seqs, chunks=chunks, sub=sub),
        "window",
        30,
        4 * cached.size * cols,
        nbytes(cached, wk, wv, wi),
        out_shape=(out, pltpu.HBM(out.shape, BF16), jax.ShapeDtypeStruct(wi.shape, BF16)),
        in_specs=[HBM_SPEC] * 6,
        out_specs=(VMEM_SPEC, HBM_SPEC, VMEM_SPEC),
        scratch_shapes=[
            pltpu.VMEM(flat.shape, BF16),
            pltpu.VMEM(wk.shape, BF16),
            pltpu.VMEM(wv.shape, BF16),
            pltpu.VMEM((window, cols), F32),
            pltpu.VMEM((window, cols), F32),
            pltpu.VMEM(out.shape, BF16),
            pltpu.VMEM(cosine.shape, F32),
            pltpu.VMEM(sine.shape, F32),
            sems((chunks,)),
            sems((chunks,)),
            sems((chunks,)),
            sems(((seqs - 1) * sub,)),
            sems,
            sems((2,)),
            sems((seqs,)),
        ],
    )(*map(in_hbm, (flat, wk, wv, cosine, sine, wi)))


def head_body(
    x_ref, gain_ref, tap_ref, bias_ref, past_ref, wi_ref, ws_ref, normed_ref, conv_ref, low_ref, xf
):
    count, _, part = x_ref.shape
    for n in range(count):
        xf[:, n * part : (n + 1) * part] = x_ref[n].astype(F32)
    x = xf[...]
    scale = lax.rsqrt(jnp.sum(x * x, axis=1, keepdims=True) / x.shape[1] + epsilon)
    normed = (x * scale * gain_ref[...]).astype(BF16)
    normed_ref[...] = normed
    ssm_input = dot(normed, wi_ref[...]).astype(BF16).astype(F32)
    taps = past_ref.shape[0]
    summed = bias_ref[...]
    for t in range(taps):
        summed = summed + past_ref[t].astype(F32) * tap_ref[t : t + 1, :]
    conv = silu(summed + tap_ref[taps : taps + 1, :] * ssm_input)
    conv_ref[...] = conv
    low_ref[...] = dot_t(conv.astype(BF16), ws_ref[...])


def head_stage(blocks, gain, taps, bias, past, w_in, w_state):
    count, rows, part = blocks.shape
    width, cols = w_in.shape
    if part % 128:
        blocks = blocks.transpose(1, 0, 2).reshape(1, rows, width)
    return call(
        head_body,
        "head",
        16,
        2 * rows * w_in.size,
        nbytes(w_in, w_state),
        out_shape=(
            jax.ShapeDtypeStruct((rows, width), BF16),
            jax.ShapeDtypeStruct((rows, cols), F32),
            jax.ShapeDtypeStruct((rows, w_state.shape[1]), F32),
        ),
        in_specs=[VMEM_SPEC] * 7,
        out_specs=(VMEM_SPEC,) * 3,
        scratch_shapes=[pltpu.VMEM((rows, width), F32)],
    )(blocks, gain[None], taps, bias[None], past.transpose(1, 0, 2), w_in, w_state.T)


def attention_body(
    len_ref, x_ref, wk_hbm, wv_hbm, wq_hbm, v_hbm, cos_hbm, sin_hbm, k_ref, out_ref,
    wk, wv, wq, v_ref, cos_near, sin_near, k_all, v_all, q_all, ksem, vsem, qsem, csem, nsem, *, seqs,
):
    start = lax.axis_index("seq") * seqs
    near = []
    for b in range(seqs):
        at = pl.ds(pl.multiple_of(len_ref[start + b] // 8 * 8, 8), 8)
        near.append(pltpu.make_async_copy(cos_hbm.at[at], cos_near.at[b], nsem.at[b]))
        near.append(pltpu.make_async_copy(sin_hbm.at[at], sin_near.at[b], nsem.at[seqs + b]))
    for copy in near:
        copy.start()
    pieces = ksem.shape[0]
    size = wk.shape[0] // pieces
    at = [pl.ds(c * size, size) for c in range(pieces)]
    groups = [[pltpu.make_async_copy(wq_hbm.at[at[c]], wq.at[at[c]], qsem.at[c])] for c in range(pieces)]
    groups.append([pltpu.make_async_copy(v_hbm, v_ref, csem)])
    groups += [
        [
            pltpu.make_async_copy(wk_hbm.at[at[c]], wk.at[at[c]], ksem.at[c]),
            pltpu.make_async_copy(wv_hbm.at[at[c]], wv.at[at[c]], vsem.at[c]),
        ]
        for c in range(pieces)
    ]
    loads = Loads(groups, 5)
    for c in range(pieces):
        loads.wait(c)
        term = dot(x_ref[:, c * size : (c + 1) * size], wq[at[c], :])
        q_all[...] = term if c == 0 else q_all[...] + term
    heads = q_all.shape[1] // HEAD_SIZE
    kv = k_all.shape[1] // HEAD_SIZE
    group = heads // kv
    window = k_ref.shape[0] // seqs
    for copy in near:
        copy.wait()
    fresh_row = lambda ref: jnp.concatenate(
        [ref[b, pl.ds(len_ref[start + b] % 8, 1), :] for b in range(seqs)], 0
    )
    cosine, sine = fresh_row(cos_near), fresh_row(sin_near)
    pick = lambda ref: jnp.concatenate([ref[pl.ds(start + b, 1), :] for b in range(seqs)], 0)
    q_own = pick(q_all)
    q = [rotate(q_own[:, lanes(h)], cosine, sine) for h in range(heads)]
    zero = jnp.zeros((1, HEAD_SIZE), F32)
    scale = HEAD_SIZE ** (-0.5)
    loads.wait(pieces)
    over_window = []
    for b in range(seqs):
        rows = [
            jnp.concatenate([q[h][b : b + 1] if j == h // group else zero for j in range(kv)], 1)
            for h in range(heads)
        ]
        q_b = jnp.concatenate(rows, 0).astype(BF16)
        v_b = v_ref[b * window : (b + 1) * window, :]
        scores = dot_t(q_b, k_ref[b * window : (b + 1) * window, :]) * scale
        valid = lax.broadcasted_iota(jnp.int32, scores.shape, 1) < len_ref[start + b]
        scores = jnp.where(valid, scores, -1e30)
        top = jnp.max(scores, axis=1, keepdims=True)
        weights = jnp.where(valid, jnp.exp(scores - top), 0.0)
        coarse = weights.astype(BF16)
        fine = (weights - coarse.astype(F32)).astype(BF16)
        mixed = dot(coarse, v_b) + dot(fine, v_b)
        over_window.append((q_b.astype(F32), top, jnp.sum(weights, axis=1, keepdims=True), mixed))
    for c in range(pieces):
        loads.wait(pieces + 1 + c)
        x = x_ref[:, c * size : (c + 1) * size]
        for total, w in ((k_all, wk), (v_all, wv)):
            term = dot(x, w[at[c], :])
            total[...] = term if c == 0 else total[...] + term
    k_own, v_own = pick(k_all), pick(v_all)
    fresh = [rotate(k_own[:, lanes(j)], cosine, sine) for j in range(kv)]
    fresh_k = jnp.concatenate(fresh, 1).astype(BF16).astype(F32)
    fresh_v = v_own.astype(BF16).astype(F32)
    for b in range(seqs):
        q_b, window_top, window_total, mixed = over_window[b]
        fresh_score = jnp.sum(q_b * fresh_k[b : b + 1], axis=1, keepdims=True) * scale
        top = jnp.maximum(window_top, fresh_score)
        kept = jnp.exp(window_top - top)
        weight_new = jnp.exp(fresh_score - top)
        mixed = (mixed * kept + weight_new * fresh_v[b : b + 1]) / (window_total * kept + weight_new)
        for h in range(heads):
            out_ref[h * seqs + b : h * seqs + b + 1, :] = mixed[h : h + 1, lanes(h // group)]


def attention_stage(lengths, normed, wq, wk, wv, keys, values, cosine, sine):
    seqs = lengths.shape[0] // lax.axis_size("seq")
    rows = normed.shape[0]
    pieces = 4
    sems = pltpu.SemaphoreType.DMA
    return call(
        functools.partial(attention_body, seqs=seqs),
        "attention",
        16,
        2 * rows * (wq.size + wk.size + wv.size) + 8 * keys.size,
        nbytes(wq, wk, wv, keys, values),
        out_shape=jax.ShapeDtypeStruct((seqs * wq.shape[1] // HEAD_SIZE, HEAD_SIZE), F32),
        in_specs=[SMEM_SPEC, VMEM_SPEC] + [HBM_SPEC] * 6 + [VMEM_SPEC],
        out_specs=VMEM_SPEC,
        scratch_shapes=[
            pltpu.VMEM(wk.shape, BF16),
            pltpu.VMEM(wv.shape, BF16),
            pltpu.VMEM(wq.shape, BF16),
            pltpu.VMEM(values.shape, BF16),
            pltpu.VMEM((seqs, 8, HEAD_SIZE), F32),
            pltpu.VMEM((seqs, 8, HEAD_SIZE), F32),
            pltpu.VMEM((rows, wk.shape[1]), F32),
            pltpu.VMEM((rows, wv.shape[1]), F32),
            pltpu.VMEM((rows, wq.shape[1]), F32),
            sems((pieces,)),
            sems((pieces,)),
            sems((pieces,)),
            sems,
            sems((2 * seqs,)),
        ],
    )(in_hbm(lengths), normed, *map(in_hbm, (wk, wv, wq, values, cosine, sine)), keys)


def pack_body(*refs, rank):
    parts = [ref[...] for ref in refs[:-3]]
    attended_ref, out_ref, buf = refs[-3:]
    while len(parts) > 1:
        parts = [sum(parts[n : n + 2]) for n in range(0, len(parts), 2)]
    batch, width = parts[0].shape
    maps = parts[0][:, rank:]
    buf[...] = jnp.zeros_like(buf)
    buf[:batch, :width] = parts[0]
    buf[:batch, width : 2 * width - rank] = maps - maps.astype(BF16).astype(F32)
    buf[: attended_ref.shape[0], buf.shape[1] - HEAD_SIZE :] = attended_ref[...]
    out_ref[...] = jnp.broadcast_to(buf[...].astype(BF16)[None], out_ref.shape)


def pack_stage(parts, attended, count, rank):
    batch, width = parts[0].shape
    rows = max(batch, -(-attended.shape[0] // 8) * 8)
    cols = -(-(2 * width - rank) // 128) * 128 + HEAD_SIZE
    return call(
        functools.partial(pack_body, rank=rank),
        "pack",
        16,
        parts[0].size,
        nbytes(*parts),
        out_shape=jax.ShapeDtypeStruct((count, rows, cols), BF16),
        in_specs=[VMEM_SPEC] * (len(parts) + 1),
        out_specs=VMEM_SPEC,
        scratch_shapes=[pltpu.VMEM((rows, cols), F32)],
    )(*parts, attended)


def mlp_body(
    x_ref, ws_hbm, wg_hbm, wu_hbm, wd_hbm, wo_hbm, st_hbm, state_hbm, skip_hbm, bias_hbm, decay_hbm, conv_ref,
    gain_ref, direct_ref, aux_ref, out_ref, wo, st, state,
    ws, wg, wu, wd, skip_ref, bias_ref, decay_ref, g_all, u_all, ssem, gsem, usem, dsem, osem,
):
    small = [
        pltpu.make_async_copy(skip_hbm, skip_ref, osem.at[3]),
        pltpu.make_async_copy(bias_hbm, bias_ref, osem.at[4]),
        pltpu.make_async_copy(decay_hbm, decay_ref, osem.at[5]),
    ]
    for copy in small:
        copy.start()
    width = x_ref.shape[1]
    inner = wg.shape[0]
    pieces = gsem.shape[0]
    chunks = dsem.shape[0]
    size = width // chunks
    part = inner // pieces
    cut = lambda n, step: pl.ds(n * step, step)
    groups = [
        [pltpu.make_async_copy(ws_hbm.at[cut(c, size)], ws.at[cut(c, size)], ssem.at[c])] for c in range(chunks)
    ]
    groups += [
        [
            pltpu.make_async_copy(wg_hbm.at[cut(n, part)], wg.at[cut(n, part)], gsem.at[n]),
            pltpu.make_async_copy(wu_hbm.at[cut(n, part)], wu.at[cut(n, part)], usem.at[n]),
        ]
        for n in range(pieces)
    ]
    groups += [
        [pltpu.make_async_copy(wd_hbm.at[:, cut(c, size)], wd.at[:, cut(c, size)], dsem.at[c])]
        for c in range(chunks)
    ]
    groups.append([pltpu.make_async_copy(state_hbm, state, osem.at[0])])
    groups.append([pltpu.make_async_copy(st_hbm, st, osem.at[1])])
    groups.append([pltpu.make_async_copy(wo_hbm, wo, osem.at[2])])
    loads = Loads(groups, 6)
    gate = None
    for c in range(chunks):
        loads.wait(c)
        term = dot(x_ref[:, cut(c, size)], ws[cut(c, size), :])
        gate = term if gate is None else gate + term
    gain_ref[...] = silu(gate)
    for copy in small:
        copy.wait()
    states = decay_ref.shape[0]
    aux_ref[:states, :] = jnp.exp(decay_ref[...])
    aux_ref[states:, :] = jnp.broadcast_to(bias_ref[...], (8, bias_ref.shape[1]))
    direct_ref[...] = skip_ref[...] * conv_ref[...]
    x = x_ref[...]
    for n in range(pieces):
        loads.wait(chunks + n)
        g_all[cut(n, part), :] = dot_t(wg[cut(n, part), :], x)
        u_all[cut(n, part), :] = dot_t(wu[cut(n, part), :], x)
    hidden = (silu(g_all[...]) * u_all[...]).T.astype(BF16)
    for c in range(chunks):
        loads.wait(chunks + pieces + c)
        out_ref[:, cut(c, size)] = dot(hidden, wd[:, cut(c, size)])
    for n in range(3):
        loads.wait(2 * chunks + pieces + n)


def mlp_stage(normed, ws, wg, wu, wd, wo, st, state, conv, skip, bias, decay):
    rows, width = normed.shape
    wg, wu = wg.T, wu.T
    inner, cols = wg.shape[0], ws.shape[1]
    pieces, chunks = pieces_of(inner, 4), 4
    like = lambda a: jax.ShapeDtypeStruct(a.shape, a.dtype)
    sems = pltpu.SemaphoreType.DMA
    return call(
        mlp_body,
        "mlp",
        24,
        2 * rows * (ws.size + wg.size + wu.size + wd.size),
        nbytes(ws, wg, wu, wd, wo),
        out_shape=(
            like(conv),
            like(conv),
            jax.ShapeDtypeStruct((decay.shape[0] + 8, cols), F32),
            jax.ShapeDtypeStruct((rows, width), F32),
            like(wo),
            like(st),
            like(state),
        ),
        in_specs=[VMEM_SPEC] + [HBM_SPEC] * 10 + [VMEM_SPEC],
        out_specs=(VMEM_SPEC,) * 7,
        scratch_shapes=[
            pltpu.VMEM(ws.shape, BF16),
            pltpu.VMEM(wg.shape, BF16),
            pltpu.VMEM(wu.shape, BF16),
            pltpu.VMEM(wd.shape, BF16),
            pltpu.VMEM((1, cols), F32),
            pltpu.VMEM((1, cols), F32),
            pltpu.VMEM(decay.shape, F32),
            pltpu.VMEM((inner, rows), F32),
            pltpu.VMEM((inner, rows), F32),
            sems((chunks,)),
            sems((pieces,)),
            sems((pieces,)),
            sems((chunks,)),
            sems((6,)),
        ],
    )(normed, *map(in_hbm, (ws, wg, wu, wd, wo, st, state, skip[None], bias[None], decay)), conv)


def tail_body(
    pack_ref, aux_ref, conv_ref, gain_ref, direct_ref, other_ref, st_ref, state, wo_ref, wa_hbm,
    state_out, term_ref, total, rows_f, wa, sem, *, seqs, heads,
):
    load = pltpu.make_async_copy(wa_hbm, wa, sem)
    load.start()
    rank = st_ref.shape[0]
    states = aux_ref.shape[0] - 8
    batch = conv_ref.shape[0]
    groups = pack_ref.shape[0]
    width = rank + 2 * states
    low = jnp.zeros((batch, width + 2 * states), F32)
    for n in range(groups):
        rows = pack_ref[n].astype(F32)
        low += rows[:batch, : width + 2 * states]
        beside = rows[:, rows.shape[1] - HEAD_SIZE :]
        for h in range(heads):
            rows_f[n * seqs : (n + 1) * seqs, lanes(h)] = beside[h * seqs : (h + 1) * seqs]
    maps = low[:, rank:].T
    maps = maps[: 2 * states] + maps[2 * states :]
    raw = dot(low[:, :rank].astype(BF16), st_ref[...]) + aux_ref[states : states + 1, :]
    step = jnp.maximum(raw, 0.0) + jnp.log1p(jnp.exp(-jnp.abs(raw)))
    rate = aux_ref[:states, :]
    drive = step * conv_ref[...]
    mixed = []
    for b in range(batch):
        kept = jnp.exp(-step[b : b + 1] * rate) * state[b]
        new = kept + drive[b : b + 1] * maps[:states, b : b + 1]
        state_out[b] = new
        mixed.append(jnp.sum(new * maps[states:, b : b + 1], axis=0, keepdims=True))
    gated = (jnp.concatenate(mixed, 0) + direct_ref[...]) * gain_ref[...]
    total[...] = other_ref[...] + dot(gated.astype(BF16), wo_ref[...])
    load.wait()
    cols = wa.shape[1]
    at = pl.ds(pl.multiple_of(lax.axis_index("seq") * cols, cols), cols)
    total[:, at] += dot(rows_f[...].astype(BF16), wa[...])
    count, _, part = term_ref.shape
    for n in range(count):
        term_ref[n] = total[:, n * part : (n + 1) * part].astype(BF16)


def tail_stage(packed, aux, conv, gain, direct, other, st, state, wo, wa, count):
    rows, width = other.shape
    seqs = rows // packed.shape[0]
    inner = wa.shape[0]
    sent, part = count, width // count
    if part % 128:
        sent, part = 1, width
    return call(
        functools.partial(tail_body, seqs=seqs, heads=inner // HEAD_SIZE),
        "tail",
        16,
        2 * rows * wo.size,
        nbytes(wo, state, state),
        out_shape=(
            jax.ShapeDtypeStruct(state.shape, F32),
            jax.ShapeDtypeStruct((sent, rows, part), BF16),
        ),
        in_specs=[VMEM_SPEC] * 9 + [HBM_SPEC],
        out_specs=(VMEM_SPEC, VMEM_SPEC),
        scratch_shapes=[
            pltpu.VMEM((rows, width), F32),
            pltpu.VMEM((rows, inner), F32),
            pltpu.VMEM(wa.shape, BF16),
            pltpu.SemaphoreType.DMA,
        ],
    )(packed, aux, conv, gain, direct, other, st, state, wo, in_hbm(wa))


def spread_body(x_ref, out_ref):
    out_ref[...] = jnp.broadcast_to(x_ref[...][None], out_ref.shape)


def spread_stage(own, count):
    return call(
        spread_body, "spread", 4, 0, 0,
        out_shape=jax.ShapeDtypeStruct((count,) + own.shape, own.dtype),
    )(own)


def close_body(own_ref, blocks_ref, out_ref):
    total = own_ref[...].astype(F32)
    parts = [blocks_ref[n].astype(F32) for n in range(blocks_ref.shape[0])]
    while len(parts) > 1:
        parts = [sum(parts[n : n + 2]) for n in range(0, len(parts), 2)]
    out_ref[...] = (total + parts[0]).astype(out_ref.dtype)


def close_stage(own, blocks):
    return call(
        close_body, "close", 4, blocks.size, 0,
        out_shape=jax.ShapeDtypeStruct(own.shape, own.dtype),
    )(own, blocks)


def gather_blocks(own):
    return lax.all_to_all(spread_stage(own, lax.axis_size(BOTH)), BOTH, 0, 0)


def exchange(value, axis, step):
    return lax.ppermute(value, axis, [(i, i ^ step) for i in range(lax.axis_size(axis))])


def per_device(
    hidden_in,
    norm_gain,
    w_ssm_in,
    w_ssm_gate,
    conv_weight,
    conv_bias,
    conv_state,
    w_state_proj,
    w_step,
    step_bias,
    log_decay,
    skip_gain,
    ssm_state,
    w_ssm_out,
    w_query,
    key_projection,
    value_projection,
    w_attn_out,
    w_mlp_gate,
    w_mlp_up,
    w_mlp_down,
    cached_inputs,
    window_lengths,
):
    batch_rows = hidden_in.shape[0]
    count = lax.axis_size(BOTH)
    blocks = gather_blocks(hidden_in)
    cosine, sine = map(jnp.asarray, rope_tables(cached_inputs.shape[1] + 8))
    keys, values, wi = window_stage(cached_inputs, key_projection, value_projection, w_ssm_in, cosine, sine)
    blocks, keys = lax.optimization_barrier((blocks, keys))
    normed, conv_out, low_part = head_stage(
        blocks, norm_gain, conv_weight, conv_bias, conv_state, wi, w_state_proj
    )
    low_parts = [low_part] + [exchange(low_part, "grp", n) for n in range(1, lax.axis_size("grp"))]
    attended = attention_stage(
        window_lengths, normed, w_query, key_projection, value_projection, keys, values, cosine, sine
    )
    packed = pack_stage(low_parts, attended, lax.axis_size("seq"), w_step.shape[0])
    packed, normed = lax.optimization_barrier((packed, normed))
    received = lax.all_to_all(packed, "seq", 0, 0)
    gain, direct, aux, other, wo, st, state = mlp_stage(
        normed, w_ssm_gate, w_mlp_gate, w_mlp_up, w_mlp_down, w_ssm_out, w_step, ssm_state,
        conv_out, skip_gain, step_bias, log_decay,
    )
    state_out, terms = tail_stage(
        received, aux, conv_out, gain, direct, other, st, state, wo, w_attn_out, count
    )
    if terms.shape[0] != count:
        terms = terms.reshape(batch_rows, count, -1).transpose(1, 0, 2)
    hidden_out = close_stage(hidden_in, lax.all_to_all(terms, BOTH, 0, 0))
    return (hidden_out, state_out)


def solution(mesh):
    placed = (
        P(None, ("grp", "seq")),
        P(),
        P(None, ("grp", "seq")),
        P(None, ("grp", "seq")),
        P(None, ("grp", "seq")),
        P(("grp", "seq")),
        P(None, None, ("grp", "seq")),
        P(("grp", "seq"), None),
        P(None, ("grp", "seq")),
        P(("grp", "seq")),
        P(None, ("grp", "seq")),
        P(("grp", "seq")),
        P(None, None, ("grp", "seq")),
        P(("grp", "seq"), None),
        P(None, "grp"),
        P(None, "grp"),
        P(None, "grp"),
        P("grp", "seq"),
        P(None, ("grp", "seq")),
        P(None, ("grp", "seq")),
        P(("grp", "seq"), None),
        P("seq", None, None),
        P(),
    )
    return jax.shard_map(
        per_device,
        mesh=mesh,
        in_specs=placed,
        out_specs=(P(None, ("grp", "seq")), P(None, None, ("grp", "seq"))),
        check_vma=False,
    )
```

```python
import functools

import jax
import jax.numpy as jnp
import numpy as np
from jax import lax
from jax.experimental import pallas as pl
from jax.experimental.pallas import tpu as pltpu
from jax.sharding import PartitionSpec as P

HEAD_SIZE = 128
BOTH = ("grp", "seq")
F32 = jnp.float32
BF16 = jnp.bfloat16

epsilon = 1e-05
rope_base = 10000.0


def rope_frequency():
    half = HEAD_SIZE // 2
    return rope_base ** (-(np.arange(half, dtype=np.float64) * 2.0) / HEAD_SIZE)


def rope_tables(count):
    angles = np.arange(count, dtype=np.float64)[:, None] * rope_frequency()[None]
    cosine, sine = np.cos(angles), np.sin(angles)
    return (
        np.concatenate([cosine, cosine], 1).astype(np.float32),
        np.concatenate([-sine, sine], 1).astype(np.float32),
    )


def rotate(head, cosine, sine):
    return head * cosine + pltpu.roll(head, HEAD_SIZE // 2, 1) * sine


def lanes(h):
    return slice(h * HEAD_SIZE, (h + 1) * HEAD_SIZE)


VMEM_SPEC = pl.BlockSpec(memory_space=pltpu.VMEM)
HBM_SPEC = pl.BlockSpec(memory_space=pltpu.HBM)
SMEM_SPEC = pl.BlockSpec(memory_space=pltpu.SMEM)


def call(body, name, vmem_mib, flops, moved, **kwargs):
    return pl.pallas_call(
        body,
        name=name,
        compiler_params=pltpu.CompilerParams(vmem_limit_bytes=vmem_mib << 20),
        cost_estimate=pl.CostEstimate(flops=int(flops), transcendentals=0, bytes_accessed=int(moved)),
        **kwargs,
    )


def in_hbm(array):
    return pltpu.with_memory_space_constraint(array, pltpu.HBM)


def dot(a, b):
    return jnp.dot(a, b, preferred_element_type=F32)


def dot_t(a, b):
    return lax.dot_general(a, b, (((1,), (1,)), ((), ())), preferred_element_type=F32)


class Loads:
    def __init__(self, groups, depth, most=None):
        self.groups, self.started = groups, 0
        self.ahead = (most or depth) - depth
        for _ in range(depth):
            self.start_next()

    def start_next(self):
        if self.started < len(self.groups):
            for copy in self.groups[self.started]:
                copy.start()
            self.started += 1

    def wait(self, n):
        for copy in self.groups[n]:
            copy.wait()
        self.start_next()
        if self.ahead > 0:
            self.ahead -= 1
            self.start_next()


def pieces_of(size, most, step=16):
    while size % most or (size // most) % step:
        most //= 2
    return most


def silu(v):
    return v / (1.0 + jnp.exp(-v))


def nbytes(*arrays):
    return sum(a.size * a.dtype.itemsize for a in arrays)


def window_body(
    x_hbm, wk_hbm, wv_hbm, cos_hbm, sin_hbm, wi_hbm,
    k_ref, v_hbm, wi,
    x, wk, wv, k_sum, v_sum, v_ref, cos_ref, sin_ref, xsem, ksem, vsem, rsem, isem, tsem, osem, *, seqs, chunks, sub,
):
    rows = k_sum.shape[0]
    width = x.shape[1]
    size = width // chunks
    groups = []
    for c in range(chunks):
        at = pl.ds(c * size, size)
        groups.append(
            [
                pltpu.make_async_copy(x_hbm.at[pl.ds(0, rows), at], x.at[pl.ds(0, rows), at], xsem.at[c]),
                pltpu.make_async_copy(wk_hbm.at[at], wk.at[at], ksem.at[c]),
                pltpu.make_async_copy(wv_hbm.at[at], wv.at[at], vsem.at[c]),
            ]
        )
    groups[1] += [
        pltpu.make_async_copy(cos_hbm, cos_ref, tsem.at[0]),
        pltpu.make_async_copy(sin_hbm, sin_ref, tsem.at[1]),
    ]
    part = rows // sub
    for n in range((seqs - 1) * sub):
        at = pl.ds(rows + n * part, part)
        groups.append([pltpu.make_async_copy(x_hbm.at[at], x.at[at], rsem.at[n])])
    groups.append([pltpu.make_async_copy(wi_hbm, wi, isem)])
    loads = Loads(groups, *WINDOW_DEPTH)

    def finish(b, k, v):
        at = slice(b * rows, (b + 1) * rows)
        for h in range(k.shape[1] // HEAD_SIZE):
            turned = rotate(k[:, lanes(h)], cos_ref[:rows, :], sin_ref[:rows, :])
            k_ref[at, lanes(h)] = turned.astype(BF16)
        v_ref[at, :] = v.astype(BF16)
        store = pltpu.make_async_copy(v_ref.at[at], v_hbm.at[at], osem.at[b])
        store.start()
        return store

    for c in range(chunks):
        loads.wait(c)
        at = slice(c * size, (c + 1) * size)
        for total, w in ((k_sum, wk), (v_sum, wv)):
            term = dot(x[:rows, at], w[at, :])
            total[...] = term if c == 0 else total[...] + term
    stores = [finish(0, k_sum[...], v_sum[...])]
    for b in range(1, seqs):
        for n in range(sub):
            loads.wait(chunks + (b - 1) * sub + n)
        own = x[b * rows : (b + 1) * rows, :]
        stores.append(finish(b, dot(own, wk[...]), dot(own, wv[...])))
    loads.wait(len(groups) - 1)
    for store in stores:
        store.wait()


WINDOW_DEPTH = (4, 5)
WINDOW_CUTS = (4, 2)


def window_stage(cached, wk, wv, wi, cosine, sine):
    seqs, window, width = cached.shape
    cols = wk.shape[1]
    chunks, sub = WINDOW_CUTS
    flat = cached.reshape(seqs * window, width)
    out = jax.ShapeDtypeStruct((seqs * window, cols), BF16)
    sems = pltpu.SemaphoreType.DMA
    return call(
        functools.partial(window_body, seqs=seqs, chunks=chunks, sub=sub),
        "window",
        30,
        4 * cached.size * cols,
        nbytes(cached, wk, wv, wi),
        out_shape=(out, pltpu.HBM(out.shape, BF16), jax.ShapeDtypeStruct(wi.shape, BF16)),
        in_specs=[HBM_SPEC] * 6,
        out_specs=(VMEM_SPEC, HBM_SPEC, VMEM_SPEC),
        scratch_shapes=[
            pltpu.VMEM(flat.shape, BF16),
            pltpu.VMEM(wk.shape, BF16),
            pltpu.VMEM(wv.shape, BF16),
            pltpu.VMEM((window, cols), F32),
            pltpu.VMEM((window, cols), F32),
            pltpu.VMEM(out.shape, BF16),
            pltpu.VMEM(cosine.shape, F32),
            pltpu.VMEM(sine.shape, F32),
            sems((chunks,)),
            sems((chunks,)),
            sems((chunks,)),
            sems(((seqs - 1) * sub,)),
            sems,
            sems((2,)),
            sems((seqs,)),
        ],
    )(*map(in_hbm, (flat, wk, wv, cosine, sine, wi)))


def head_body(
    x_ref, gain_ref, tap_ref, bias_ref, past_ref, wi_ref, ws_ref, normed_ref, conv_ref, low_ref, xf
):
    count, _, part = x_ref.shape
    for n in range(count):
        xf[:, n * part : (n + 1) * part] = x_ref[n].astype(F32)
    x = xf[...]
    scale = lax.rsqrt(jnp.sum(x * x, axis=1, keepdims=True) / x.shape[1] + epsilon)
    normed = (x * scale * gain_ref[...]).astype(BF16)
    normed_ref[...] = normed
    ssm_input = dot(normed, wi_ref[...]).astype(BF16).astype(F32)
    taps = past_ref.shape[0]
    summed = bias_ref[...]
    for t in range(taps):
        summed = summed + past_ref[t].astype(F32) * tap_ref[t : t + 1, :]
    conv = silu(summed + tap_ref[taps : taps + 1, :] * ssm_input)
    conv_ref[...] = conv
    low_ref[...] = dot_t(conv.astype(BF16), ws_ref[...])


def head_stage(blocks, gain, taps, bias, past, w_in, w_state):
    count, rows, part = blocks.shape
    width, cols = w_in.shape
    if part % 128:
        blocks = blocks.transpose(1, 0, 2).reshape(1, rows, width)
    return call(
        head_body,
        "head",
        16,
        2 * rows * w_in.size,
        nbytes(w_in, w_state),
        out_shape=(
            jax.ShapeDtypeStruct((rows, width), BF16),
            jax.ShapeDtypeStruct((rows, cols), F32),
            jax.ShapeDtypeStruct((rows, w_state.shape[1]), F32),
        ),
        in_specs=[VMEM_SPEC] * 7,
        out_specs=(VMEM_SPEC,) * 3,
        scratch_shapes=[pltpu.VMEM((rows, width), F32)],
    )(blocks, gain[None], taps, bias[None], past.transpose(1, 0, 2), w_in, w_state.T)


def attention_body(
    len_ref, x_ref, wk_hbm, wv_hbm, wq_hbm, v_hbm, cos_hbm, sin_hbm, k_ref, out_ref,
    wk, wv, wq, v_ref, cos_near, sin_near, k_all, v_all, q_all, ksem, vsem, qsem, csem, nsem, *, seqs,
):
    start = lax.axis_index("seq") * seqs
    near = []
    for b in range(seqs):
        at = pl.ds(pl.multiple_of(len_ref[start + b] // 8 * 8, 8), 8)
        near.append(pltpu.make_async_copy(cos_hbm.at[at], cos_near.at[b], nsem.at[b]))
        near.append(pltpu.make_async_copy(sin_hbm.at[at], sin_near.at[b], nsem.at[seqs + b]))
    for copy in near:
        copy.start()
    pieces = ksem.shape[0]
    size = wk.shape[0] // pieces
    at = [pl.ds(c * size, size) for c in range(pieces)]
    groups = [[pltpu.make_async_copy(wq_hbm.at[at[c]], wq.at[at[c]], qsem.at[c])] for c in range(pieces)]
    groups.append([pltpu.make_async_copy(v_hbm, v_ref, csem)])
    groups += [
        [
            pltpu.make_async_copy(wk_hbm.at[at[c]], wk.at[at[c]], ksem.at[c]),
            pltpu.make_async_copy(wv_hbm.at[at[c]], wv.at[at[c]], vsem.at[c]),
        ]
        for c in range(pieces)
    ]
    loads = Loads(groups, 5)
    for c in range(pieces):
        loads.wait(c)
        term = dot(x_ref[:, c * size : (c + 1) * size], wq[at[c], :])
        q_all[...] = term if c == 0 else q_all[...] + term
    heads = q_all.shape[1] // HEAD_SIZE
    kv = k_all.shape[1] // HEAD_SIZE
    group = heads // kv
    window = k_ref.shape[0] // seqs
    for copy in near:
        copy.wait()
    fresh_row = lambda ref: jnp.concatenate(
        [ref[b, pl.ds(len_ref[start + b] % 8, 1), :] for b in range(seqs)], 0
    )
    cosine, sine = fresh_row(cos_near), fresh_row(sin_near)
    pick = lambda ref: jnp.concatenate([ref[pl.ds(start + b, 1), :] for b in range(seqs)], 0)
    q_own = pick(q_all)
    q = [rotate(q_own[:, lanes(h)], cosine, sine) for h in range(heads)]
    zero = jnp.zeros((1, HEAD_SIZE), F32)
    scale = HEAD_SIZE ** (-0.5)
    loads.wait(pieces)
    over_window = []
    for b in range(seqs):
        rows = [
            jnp.concatenate([q[h][b : b + 1] if j == h // group else zero for j in range(kv)], 1)
            for h in range(heads)
        ]
        q_b = jnp.concatenate(rows, 0).astype(BF16)
        v_b = v_ref[b * window : (b + 1) * window, :]
        scores = dot_t(q_b, k_ref[b * window : (b + 1) * window, :]) * scale
        valid = lax.broadcasted_iota(jnp.int32, scores.shape, 1) < len_ref[start + b]
        scores = jnp.where(valid, scores, -1e30)
        top = jnp.max(scores, axis=1, keepdims=True)
        weights = jnp.where(valid, jnp.exp(scores - top), 0.0)
        coarse = weights.astype(BF16)
        fine = (weights - coarse.astype(F32)).astype(BF16)
        mixed = dot(coarse, v_b) + dot(fine, v_b)
        over_window.append((q_b.astype(F32), top, jnp.sum(weights, axis=1, keepdims=True), mixed))
    for c in range(pieces):
        loads.wait(pieces + 1 + c)
        x = x_ref[:, c * size : (c + 1) * size]
        for total, w in ((k_all, wk), (v_all, wv)):
            term = dot(x, w[at[c], :])
            total[...] = term if c == 0 else total[...] + term
    k_own, v_own = pick(k_all), pick(v_all)
    fresh = [rotate(k_own[:, lanes(j)], cosine, sine) for j in range(kv)]
    fresh_k = jnp.concatenate(fresh, 1).astype(BF16).astype(F32)
    fresh_v = v_own.astype(BF16).astype(F32)
    for b in range(seqs):
        q_b, window_top, window_total, mixed = over_window[b]
        fresh_score = jnp.sum(q_b * fresh_k[b : b + 1], axis=1, keepdims=True) * scale
        top = jnp.maximum(window_top, fresh_score)
        kept = jnp.exp(window_top - top)
        weight_new = jnp.exp(fresh_score - top)
        mixed = (mixed * kept + weight_new * fresh_v[b : b + 1]) / (window_total * kept + weight_new)
        for h in range(heads):
            out_ref[h * seqs + b : h * seqs + b + 1, :] = mixed[h : h + 1, lanes(h // group)]


def attention_stage(lengths, normed, wq, wk, wv, keys, values, cosine, sine):
    seqs = lengths.shape[0] // lax.axis_size("seq")
    rows = normed.shape[0]
    pieces = 4
    sems = pltpu.SemaphoreType.DMA
    return call(
        functools.partial(attention_body, seqs=seqs),
        "attention",
        16,
        2 * rows * (wq.size + wk.size + wv.size) + 8 * keys.size,
        nbytes(wq, wk, wv, keys, values),
        out_shape=jax.ShapeDtypeStruct((seqs * wq.shape[1] // HEAD_SIZE, HEAD_SIZE), F32),
        in_specs=[SMEM_SPEC, VMEM_SPEC] + [HBM_SPEC] * 6 + [VMEM_SPEC],
        out_specs=VMEM_SPEC,
        scratch_shapes=[
            pltpu.VMEM(wk.shape, BF16),
            pltpu.VMEM(wv.shape, BF16),
            pltpu.VMEM(wq.shape, BF16),
            pltpu.VMEM(values.shape, BF16),
            pltpu.VMEM((seqs, 8, HEAD_SIZE), F32),
            pltpu.VMEM((seqs, 8, HEAD_SIZE), F32),
            pltpu.VMEM((rows, wk.shape[1]), F32),
            pltpu.VMEM((rows, wv.shape[1]), F32),
            pltpu.VMEM((rows, wq.shape[1]), F32),
            sems((pieces,)),
            sems((pieces,)),
            sems((pieces,)),
            sems,
            sems((2 * seqs,)),
        ],
    )(in_hbm(lengths), normed, *map(in_hbm, (wk, wv, wq, values, cosine, sine)), keys)


def pack_body(*refs, rank):
    parts = [ref[...] for ref in refs[:-3]]
    attended_ref, out_ref, buf = refs[-3:]
    while len(parts) > 1:
        parts = [sum(parts[n : n + 2]) for n in range(0, len(parts), 2)]
    batch, width = parts[0].shape
    maps = parts[0][:, rank:]
    buf[...] = jnp.zeros_like(buf)
    buf[:batch, :width] = parts[0]
    buf[:batch, width : 2 * width - rank] = maps - maps.astype(BF16).astype(F32)
    buf[: attended_ref.shape[0], buf.shape[1] - HEAD_SIZE :] = attended_ref[...]
    out_ref[...] = jnp.broadcast_to(buf[...].astype(BF16)[None], out_ref.shape)


def pack_stage(parts, attended, count, rank):
    batch, width = parts[0].shape
    rows = max(batch, -(-attended.shape[0] // 8) * 8)
    cols = -(-(2 * width - rank) // 128) * 128 + HEAD_SIZE
    return call(
        functools.partial(pack_body, rank=rank),
        "pack",
        16,
        parts[0].size,
        nbytes(*parts),
        out_shape=jax.ShapeDtypeStruct((count, rows, cols), BF16),
        in_specs=[VMEM_SPEC] * (len(parts) + 1),
        out_specs=VMEM_SPEC,
        scratch_shapes=[pltpu.VMEM((rows, cols), F32)],
    )(*parts, attended)


def mlp_body(
    x_ref, ws_hbm, wg_hbm, wu_hbm, wd_hbm, wo_hbm, st_hbm, state_hbm, skip_hbm, bias_hbm, decay_hbm, conv_ref,
    gain_ref, direct_ref, aux_ref, out_ref, wo, st, state,
    ws, wg, wu, wd, skip_ref, bias_ref, decay_ref, g_all, u_all, ssem, gsem, usem, dsem, osem,
):
    small = [
        pltpu.make_async_copy(skip_hbm, skip_ref, osem.at[3]),
        pltpu.make_async_copy(bias_hbm, bias_ref, osem.at[4]),
        pltpu.make_async_copy(decay_hbm, decay_ref, osem.at[5]),
    ]
    for copy in small:
        copy.start()
    width = x_ref.shape[1]
    inner = wg.shape[0]
    pieces = gsem.shape[0]
    chunks = dsem.shape[0]
    size = width // chunks
    part = inner // pieces
    cut = lambda n, step: pl.ds(n * step, step)
    groups = [
        [pltpu.make_async_copy(ws_hbm.at[cut(c, size)], ws.at[cut(c, size)], ssem.at[c])] for c in range(chunks)
    ]
    groups += [
        [
            pltpu.make_async_copy(wg_hbm.at[cut(n, part)], wg.at[cut(n, part)], gsem.at[n]),
            pltpu.make_async_copy(wu_hbm.at[cut(n, part)], wu.at[cut(n, part)], usem.at[n]),
        ]
        for n in range(pieces)
    ]
    groups += [
        [pltpu.make_async_copy(wd_hbm.at[:, cut(c, size)], wd.at[:, cut(c, size)], dsem.at[c])]
        for c in range(chunks)
    ]
    groups.append([pltpu.make_async_copy(state_hbm, state, osem.at[0])])
    groups.append([pltpu.make_async_copy(st_hbm, st, osem.at[1])])
    groups.append([pltpu.make_async_copy(wo_hbm, wo, osem.at[2])])
    loads = Loads(groups, 5)
    gate = None
    for c in range(chunks):
        loads.wait(c)
        term = dot(x_ref[:, cut(c, size)], ws[cut(c, size), :])
        gate = term if gate is None else gate + term
    gain_ref[...] = silu(gate)
    for copy in small:
        copy.wait()
    states = decay_ref.shape[0]
    aux_ref[:states, :] = jnp.exp(decay_ref[...])
    aux_ref[states:, :] = jnp.broadcast_to(bias_ref[...], (8, bias_ref.shape[1]))
    direct_ref[...] = skip_ref[...] * conv_ref[...]
    x = x_ref[...]
    for n in range(pieces):
        loads.wait(chunks + n)
        g_all[cut(n, part), :] = dot_t(wg[cut(n, part), :], x)
        u_all[cut(n, part), :] = dot_t(wu[cut(n, part), :], x)
    hidden = (silu(g_all[...]) * u_all[...]).T.astype(BF16)
    for c in range(chunks):
        loads.wait(chunks + pieces + c)
        out_ref[:, cut(c, size)] = dot(hidden, wd[:, cut(c, size)])
    for n in range(3):
        loads.wait(2 * chunks + pieces + n)


def mlp_stage(normed, ws, wg, wu, wd, wo, st, state, conv, skip, bias, decay):
    rows, width = normed.shape
    wg, wu = wg.T, wu.T
    inner, cols = wg.shape[0], ws.shape[1]
    pieces, chunks = pieces_of(inner, 2), 2
    like = lambda a: jax.ShapeDtypeStruct(a.shape, a.dtype)
    sems = pltpu.SemaphoreType.DMA
    return call(
        mlp_body,
        "mlp",
        24,
        2 * rows * (ws.size + wg.size + wu.size + wd.size),
        nbytes(ws, wg, wu, wd, wo),
        out_shape=(
            like(conv),
            like(conv),
            jax.ShapeDtypeStruct((decay.shape[0] + 8, cols), F32),
            jax.ShapeDtypeStruct((rows, width), F32),
            like(wo),
            like(st),
            like(state),
        ),
        in_specs=[VMEM_SPEC] + [HBM_SPEC] * 10 + [VMEM_SPEC],
        out_specs=(VMEM_SPEC,) * 7,
        scratch_shapes=[
            pltpu.VMEM(ws.shape, BF16),
            pltpu.VMEM(wg.shape, BF16),
            pltpu.VMEM(wu.shape, BF16),
            pltpu.VMEM(wd.shape, BF16),
            pltpu.VMEM((1, cols), F32),
            pltpu.VMEM((1, cols), F32),
            pltpu.VMEM(decay.shape, F32),
            pltpu.VMEM((inner, rows), F32),
            pltpu.VMEM((inner, rows), F32),
            sems((chunks,)),
            sems((pieces,)),
            sems((pieces,)),
            sems((chunks,)),
            sems((6,)),
        ],
    )(normed, *map(in_hbm, (ws, wg, wu, wd, wo, st, state, skip[None], bias[None], decay)), conv)


def tail_body(
    pack_ref, aux_ref, conv_ref, gain_ref, direct_ref, other_ref, st_ref, state, wo_ref, wa_hbm,
    state_out, term_ref, total, rows_f, wa, sem, *, seqs, heads,
):
    load = pltpu.make_async_copy(wa_hbm, wa, sem)
    load.start()
    rank = st_ref.shape[0]
    states = aux_ref.shape[0] - 8
    batch = conv_ref.shape[0]
    groups = pack_ref.shape[0]
    width = rank + 2 * states
    low = jnp.zeros((batch, width + 2 * states), F32)
    for n in range(groups):
        rows = pack_ref[n].astype(F32)
        low += rows[:batch, : width + 2 * states]
        beside = rows[:, rows.shape[1] - HEAD_SIZE :]
        for h in range(heads):
            rows_f[n * seqs : (n + 1) * seqs, lanes(h)] = beside[h * seqs : (h + 1) * seqs]
    maps = low[:, rank:].T
    maps = maps[: 2 * states] + maps[2 * states :]
    raw = dot(low[:, :rank].astype(BF16), st_ref[...]) + aux_ref[states : states + 1, :]
    step = jnp.maximum(raw, 0.0) + jnp.log1p(jnp.exp(-jnp.abs(raw)))
    rate = aux_ref[:states, :]
    drive = step * conv_ref[...]
    mixed = []
    for b in range(batch):
        kept = jnp.exp(-step[b : b + 1] * rate) * state[b]
        new = kept + drive[b : b + 1] * maps[:states, b : b + 1]
        state_out[b] = new
        mixed.append(jnp.sum(new * maps[states:, b : b + 1], axis=0, keepdims=True))
    gated = (jnp.concatenate(mixed, 0) + direct_ref[...]) * gain_ref[...]
    total[...] = other_ref[...] + dot(gated.astype(BF16), wo_ref[...])
    load.wait()
    cols = wa.shape[1]
    at = pl.ds(pl.multiple_of(lax.axis_index("seq") * cols, cols), cols)
    total[:, at] += dot(rows_f[...].astype(BF16), wa[...])
    count, _, part = term_ref.shape
    for n in range(count):
        term_ref[n] = total[:, n * part : (n + 1) * part].astype(BF16)


def tail_stage(packed, aux, conv, gain, direct, other, st, state, wo, wa, count):
    rows, width = other.shape
    seqs = rows // packed.shape[0]
    inner = wa.shape[0]
    sent, part = count, width // count
    if part % 128:
        sent, part = 1, width
    return call(
        functools.partial(tail_body, seqs=seqs, heads=inner // HEAD_SIZE),
        "tail",
        16,
        2 * rows * wo.size,
        nbytes(wo, state, state),
        out_shape=(
            jax.ShapeDtypeStruct(state.shape, F32),
            jax.ShapeDtypeStruct((sent, rows, part), BF16),
        ),
        in_specs=[VMEM_SPEC] * 9 + [HBM_SPEC],
        out_specs=(VMEM_SPEC, VMEM_SPEC),
        scratch_shapes=[
            pltpu.VMEM((rows, width), F32),
            pltpu.VMEM((rows, inner), F32),
            pltpu.VMEM(wa.shape, BF16),
            pltpu.SemaphoreType.DMA,
        ],
    )(packed, aux, conv, gain, direct, other, st, state, wo, in_hbm(wa))


def spread_body(x_ref, out_ref):
    out_ref[...] = jnp.broadcast_to(x_ref[...][None], out_ref.shape)


def spread_stage(own, count):
    return call(
        spread_body, "spread", 4, 0, 0,
        out_shape=jax.ShapeDtypeStruct((count,) + own.shape, own.dtype),
    )(own)


def close_body(own_ref, blocks_ref, out_ref):
    total = own_ref[...].astype(F32)
    parts = [blocks_ref[n].astype(F32) for n in range(blocks_ref.shape[0])]
    while len(parts) > 1:
        parts = [sum(parts[n : n + 2]) for n in range(0, len(parts), 2)]
    out_ref[...] = (total + parts[0]).astype(out_ref.dtype)


def close_stage(own, blocks):
    return call(
        close_body, "close", 4, blocks.size, 0,
        out_shape=jax.ShapeDtypeStruct(own.shape, own.dtype),
    )(own, blocks)


def gather_blocks(own):
    return lax.all_to_all(spread_stage(own, lax.axis_size(BOTH)), BOTH, 0, 0)


def exchange(value, axis, step):
    return lax.ppermute(value, axis, [(i, i ^ step) for i in range(lax.axis_size(axis))])


def per_device(
    hidden_in,
    norm_gain,
    w_ssm_in,
    w_ssm_gate,
    conv_weight,
    conv_bias,
    conv_state,
    w_state_proj,
    w_step,
    step_bias,
    log_decay,
    skip_gain,
    ssm_state,
    w_ssm_out,
    w_query,
    key_projection,
    value_projection,
    w_attn_out,
    w_mlp_gate,
    w_mlp_up,
    w_mlp_down,
    cached_inputs,
    window_lengths,
):
    batch_rows = hidden_in.shape[0]
    count = lax.axis_size(BOTH)
    blocks = gather_blocks(hidden_in)
    cosine, sine = map(jnp.asarray, rope_tables(cached_inputs.shape[1] + 8))
    keys, values, wi = window_stage(cached_inputs, key_projection, value_projection, w_ssm_in, cosine, sine)
    blocks, keys = lax.optimization_barrier((blocks, keys))
    normed, conv_out, low_part = head_stage(
        blocks, norm_gain, conv_weight, conv_bias, conv_state, wi, w_state_proj
    )
    low_parts = [low_part] + [exchange(low_part, "grp", n) for n in range(1, lax.axis_size("grp"))]
    attended = attention_stage(
        window_lengths, normed, w_query, key_projection, value_projection, keys, values, cosine, sine
    )
    packed = pack_stage(low_parts, attended, lax.axis_size("seq"), w_step.shape[0])
    packed, normed = lax.optimization_barrier((packed, normed))
    received = lax.all_to_all(packed, "seq", 0, 0)
    gain, direct, aux, other, wo, st, state = mlp_stage(
        normed, w_ssm_gate, w_mlp_gate, w_mlp_up, w_mlp_down, w_ssm_out, w_step, ssm_state,
        conv_out, skip_gain, step_bias, log_decay,
    )
    state_out, terms = tail_stage(
        received, aux, conv_out, gain, direct, other, st, state, wo, w_attn_out, count
    )
    if terms.shape[0] != count:
        terms = terms.reshape(batch_rows, count, -1).transpose(1, 0, 2)
    hidden_out = close_stage(hidden_in, lax.all_to_all(terms, BOTH, 0, 0))
    return (hidden_out, state_out)


def solution(mesh):
    placed = (
        P(None, ("grp", "seq")),
        P(),
        P(None, ("grp", "seq")),
        P(None, ("grp", "seq")),
        P(None, ("grp", "seq")),
        P(("grp", "seq")),
        P(None, None, ("grp", "seq")),
        P(("grp", "seq"), None),
        P(None, ("grp", "seq")),
        P(("grp", "seq")),
        P(None, ("grp", "seq")),
        P(("grp", "seq")),
        P(None, None, ("grp", "seq")),
        P(("grp", "seq"), None),
        P(None, "grp"),
        P(None, "grp"),
        P(None, "grp"),
        P("grp", "seq"),
        P(None, ("grp", "seq")),
        P(None, ("grp", "seq")),
        P(("grp", "seq"), None),
        P("seq", None, None),
        P(),
    )
    return jax.shard_map(
        per_device,
        mesh=mesh,
        in_specs=placed,
        out_specs=(P(None, ("grp", "seq")), P(None, None, ("grp", "seq"))),
        check_vma=False,
    )
```
